16 devices in a mesh: dp: 1, tp: 16 (over x, y, z, core).
Axes of the slice: x: 2, y: 2, z: 2, core: 2. Of those that a mesh axis runs over, the one named last changes fastest.
Arguments:
- x: bfloat16 [2048, 8192], P(('dp', 'tp'))
- gain_a: bfloat16 [8192], replicated
- wq: bfloat16 [8192, 8192], P(None, 'tp')
- wk: bfloat16 [8192, 8192], P(None, 'tp')
- wv: bfloat16 [8192, 8192], P(None, 'tp')
- wo: bfloat16 [8192, 8192], P('tp')
- gain_m: bfloat16 [8192], replicated
- w_gate: bfloat16 [8192, 24576], P(None, 'tp')
- w_up: bfloat16 [8192, 24576], P(None, 'tp')
- w_down: bfloat16 [24576, 8192], P('tp')
Outputs:
- output: bfloat16 [2048, 8192], P(('dp', 'tp'))
All inputs are finite; a program needn't handle non-finite values.
Results may differ from the reference program's by a relative error of at most 0.017.
Values are sent between devices in bfloat16 or wider.
A program may use at most 2 GiB of HBM per device.

```python
import jax
import jax.numpy as jnp
from jax import lax

ROWS = 2048
D = 8192
HEADS = 64
KV_HEADS = 64
HEAD = 128
FF = 24576
THETA = 10000


def setup_inputs(seed: int = 0, part: int = 0) -> dict:
    kx, kn, kq, kk, kv, ko, km, kg, ku, kd = jax.random.split(jax.random.key(seed), 10)

    def weights(key, rows, columns):
        return jax.random.normal(key, (rows, columns), jnp.float32) * rows**-0.5

    drawn = {
        "x": jax.random.normal(jax.random.fold_in(kx, part), (ROWS, D), jnp.float32),
        "gain_a": 1 + 0.1 * jax.random.normal(kn, (D,), jnp.float32),
        "wq": 2 * weights(kq, D, HEADS * HEAD),
        "wk": 2 * weights(kk, D, KV_HEADS * HEAD),
        "wv": 4 * weights(kv, D, KV_HEADS * HEAD),
        "wo": weights(ko, HEADS * HEAD, D),
        "gain_m": 1 + 0.1 * jax.random.normal(km, (D,), jnp.float32),
        "w_gate": weights(kg, D, FF),
        "w_up": weights(ku, D, FF),
        "w_down": 2 * weights(kd, FF, D),
    }
    return {k: v.astype(jnp.bfloat16) for k, v in drawn.items()}


def normed(x, gain):
    wide = x.astype(jnp.float32)
    scale = lax.rsqrt(jnp.mean(wide * wide, -1, keepdims=True) + 1e-6)
    return (wide * scale * gain.astype(jnp.float32)).astype(jnp.bfloat16)


def turned(t, place, theta):
    half = t.shape[-1] // 2
    angle = place.astype(jnp.float32)[:, None] * theta ** (-jnp.arange(half, dtype=jnp.float32) / half)
    cos, sin = jnp.cos(angle)[:, None], jnp.sin(angle)[:, None]
    a, b = t[..., :half].astype(jnp.float32), t[..., half:].astype(jnp.float32)
    return jnp.concatenate([a * cos - b * sin, b * cos + a * sin], -1).astype(jnp.bfloat16)


def matmul(a, w):
    return jnp.dot(a, w, preferred_element_type=jnp.float32).astype(jnp.bfloat16)


def einsum(form, a, b):
    return jnp.einsum(form, a.astype(jnp.float32), b.astype(jnp.float32))


def attention(q, k, v):
    scores = einsum("tgsd,ugd->gstu", q, k) * q.shape[-1] ** -0.5
    token = jnp.arange(q.shape[0])
    scores = jnp.where(token[:, None] >= token, scores, -jnp.inf)
    weights = jax.nn.softmax(scores, -1).astype(jnp.bfloat16)
    return einsum("gstu,ugd->tgsd", weights, v).astype(jnp.bfloat16)


def reference(x, gain_a, wq, wk, wv, wo, gain_m, w_gate, w_up, w_down):
    a, place = normed(x, gain_a), jnp.arange(ROWS)
    q = turned(matmul(a, wq).reshape(ROWS, HEADS, HEAD), place, THETA).reshape(ROWS, KV_HEADS, -1, HEAD)
    k = turned(matmul(a, wk).reshape(ROWS, KV_HEADS, HEAD), place, THETA)
    v = matmul(a, wv).reshape(ROWS, KV_HEADS, HEAD)
    seen = attention(q, k, v).reshape(ROWS, HEADS * HEAD)
    h = (x.astype(jnp.float32) + jnp.dot(seen, wo, preferred_element_type=jnp.float32)).astype(jnp.bfloat16)
    b = normed(h, gain_m)
    gate = jnp.dot(b, w_gate, preferred_element_type=jnp.float32)
    up = jnp.dot(b, w_up, preferred_element_type=jnp.float32)
    hidden = (jax.nn.silu(gate) * up).astype(jnp.bfloat16)
    return (h.astype(jnp.float32) + jnp.dot(hidden, w_down, preferred_element_type=jnp.float32)).astype(jnp.bfloat16)
```

```python
import functools

import jax
import jax.numpy as jnp
from jax import lax
from jax.experimental import pallas as pl
from jax.experimental.pallas import tpu as pltpu

NEG = -1e30
HIDDEN = 2 * NEG
LOG2E = 1.4426950408889634
STRIP = 512


def _dot(a, b, ca, cb):
    return lax.dot_general(a, b, (((ca,), (cb,)), ((), ())), preferred_element_type=jnp.float32)


def _forward(q_ref, k_ref, v_ref, o_ref, top_s, mix_s, gap_s, *, scale, bk):
    kb, bq, d = q_ref.shape
    iq = pl.program_id(0)
    e = scale * LOG2E
    pieces = [(i, at) for i in range(kb) for at in range(0, bq, STRIP)]
    gap_s[...] = lax.broadcasted_iota(jnp.int32, gap_s.shape, 1) - lax.broadcasted_iota(jnp.int32, gap_s.shape, 0)
    top_s[...] = jnp.full(top_s.shape, NEG, jnp.float32)
    mix_s[...] = jnp.zeros(mix_s.shape, jnp.float32)
    ones = jnp.ones((8, bk), k_ref.dtype)

    def block(j, masked):
        here = pl.ds(j * bk, bk)
        scores = [_dot(k_ref[i, here, :], q_ref[i, at : at + STRIP, :], 1, 1) for i, at in pieces]
        weights, keeps = [], []
        for (i, at), s in zip(pieces, scores):
            if masked:
                s = jnp.where(gap_s[:, at : at + STRIP] >= j * bk - iq * bq, s, HIDDEN)
            old = top_s[i : i + 1, at : at + STRIP]
            top = jnp.maximum(old, s.max(axis=0, keepdims=True))
            top_s[i : i + 1, at : at + STRIP] = top
            weights.append(jnp.exp2((s - top) * e).astype(k_ref.dtype))
            keeps.append(jnp.exp2((old - top) * e))
        for (i, at), p, keep in zip(pieces, weights, keeps):
            values = jnp.concatenate([v_ref[i, here, :].T, ones], axis=0)
            mix_s[i, :, at : at + STRIP] = mix_s[i, :, at : at + STRIP] * keep + _dot(values, p, 1, 0)

    per = bq // bk
    lax.fori_loop(0, iq * per, lambda j, _: block(j, False), None)
    lax.fori_loop(iq * per, iq * per + per, lambda j, _: block(j, True), None)
    for i in range(kb):
        o_ref[i] = (mix_s[i, :d, :] * (1 / mix_s[i, d : d + 1, :])).T.astype(o_ref.dtype)


def attend(q, k, v, bq=1024, bk=512):
    h, s, d = q.shape
    whole = pl.BlockSpec((h, s, d), lambda iq: (0, 0, 0))
    queries = pl.BlockSpec((h, bq, d), lambda iq: (0, iq, 0))
    return pl.pallas_call(
        functools.partial(_forward, scale=d**-0.5, bk=bk),
        grid=(s // bq,),
        in_specs=[queries, whole, whole],
        out_specs=queries,
        out_shape=jax.ShapeDtypeStruct((h, s, d), q.dtype),
        scratch_shapes=[pltpu.VMEM((h, bq), jnp.float32), pltpu.VMEM((h, d + 8, bq), jnp.float32), pltpu.VMEM((bk, bq), jnp.int32)],
        compiler_params=pltpu.CompilerParams(dimension_semantics=("arbitrary",), vmem_limit_bytes=KERNEL_VMEM),
        cost_estimate=pl.CostEstimate(flops=4 * h * s * s * d, transcendentals=h * s * s, bytes_accessed=8 * h * s * d),
    )(q, k, v)


from jax.sharding import PartitionSpec as P

HEAD = 128
THETA = 10000
MESH = pl.DeviceIdType.MESH
KERNEL_VMEM = 66_000_000
X, Y, Z = 4, 2, 1
OUT = ((X, X | Y, Y), (Y, Y | Z, Z), (Z, Z | X, X))
THIRDS = ((0, 48, X | Y, Z), (48, 48, Y | Z, X), (96, 32, Z | X, Y))
HALF = 64
DEPTH = 2048
WIDE = 512


def normed(x, gain):
    wide = x.astype(jnp.float32)
    scale = lax.rsqrt(jnp.mean(wide * wide, -1, keepdims=True) + 1e-6)
    return (wide * scale * gain.astype(jnp.float32)).astype(jnp.bfloat16)


def _flip(n, bit):
    return n + bit - 2 * bit * lax.rem(lax.div(n, bit), 2)


def _flips(n, bits):
    for bit in (4, 2, 1):
        if bits & bit:
            n = _flip(n, bit)
    return n


def _places():
    me = lax.axis_index("tp")
    chip, core = lax.div(me, 2), lax.rem(me, 2)
    return chip, core, {axis: _flip(me, 2 * axis) for axis in (X, Y, Z)}, _flip(me, 1)


def _greet(partners):
    barrier = pltpu.get_barrier_semaphore()
    for partner in partners:
        pl.semaphore_signal(barrier, inc=1, device_id={"tp": partner}, device_id_type=MESH)
    pl.semaphore_wait(barrier, len(partners))


def _gather_matmul(gated, a_ref, *refs):
    if gated:
        w_refs, (out_ref, all_ref), rest = refs[:2], refs[2:4], refs[4:]
        (held, part, lhs, total, stage, w_sem, p_sem, l_sem, o_sem, send, recv, csend, crecv) = rest
    else:
        w_refs, (cos_ref, sin_ref), outs, all_ref, rest = refs[:3], refs[3:5], refs[5:8], refs[8], refs[9:]
        (held, lhs, total, stage, w_sem, l_sem, o_sem, send, recv, csend, crecv) = rest
    chip, core, near, sibling = _places()
    steps = a_ref.shape[1] // DEPTH
    tiles = 3
    count = tiles * steps

    def hop(i, src, dst, axis):
        return pltpu.make_async_remote_copy(src, dst, send.at[i], recv.at[i], device_id={"tp": near[axis]}, device_id_type=MESH)

    def across(i, src, dst):
        return pltpu.make_async_remote_copy(src, dst, csend.at[i], crecv.at[i], device_id={"tp": sibling}, device_id_type=MESH)

    def rows(unit, whose, at, n):
        return all_ref.at[unit, whose, pl.ds(at, n)]

    first, second, third, cross = {}, {}, {}, {}
    for h in range(2):
        for n, (one, two, axis) in enumerate(OUT):
            first[h, n] = hop(h * 3 + n, a_ref.at[pl.ds(h * HALF, HALF)], rows(one, core, h * HALF, HALF), one)
            second[h, n] = hop(6 + h * 3 + n, rows(one, core, h * HALF, HALF), rows(two, core, h * HALF, HALF), axis)
            cross[1 + h, n] = across(1 + h * 3 + n, rows(one, core, h * HALF, HALF), rows(one, core, h * HALF, HALF))
            cross[3 + h, n] = across(7 + h * 3 + n, rows(two, core, h * HALF, HALF), rows(two, core, h * HALF, HALF))
    for n, (at, size, source, axis) in enumerate(THIRDS):
        third[n] = hop(12 + n, rows(source, core, at, size), rows(7, core, at, size), axis)
        cross[5, n] = across(13 + n, rows(7, core, at, size), rows(7, core, at, size))
    cross[0, 0] = across(0, a_ref, rows(0, core, 0, 2 * HALF))

    ones, twos = [n[0] for n in OUT], [n[1] for n in OUT]
    blocks = [[(0, m, 0, 128) for m in (True, False)]]
    for units in (ones, twos):
        for h in range(2):
            blocks.append([(u, m, h * HALF, HALF) for m in (True, False) for u in units])
    blocks.append([(7, m, 0, 128) for m in (True, False)])

    def loads(b, mine):
        at, slot, got = 0, b % 2, []
        for n, (unit, m, row, size) in enumerate(blocks[b]):
            if m == mine:
                src = a_ref if unit == 0 and m else rows(unit, core if m else 1 - core, row, size)
                got.append(pltpu.make_async_copy(src, lhs.at[slot, pl.ds(at, size)], l_sem.at[slot, n]))
            at += size
        return got

    def arrivals(b):
        return {1: [first[0, n] for n in range(3)], 2: [first[1, n] for n in range(3)], 3: [second[0, n] for n in range(3)],
                4: [second[1, n] for n in range(3)], 5: [third[n] for n in range(3)]}[b]

    def onward(b):
        return {1: [second[0, n] for n in range(3)], 2: [second[1, n] for n in range(3)], 4: [third[n] for n in range(3)]}.get(b, [])

    def stores(b, t):
        at, got = 0, []
        for n, (unit, m, row, size) in enumerate(blocks[b]):
            whose = core if m else 1 - core
            if gated:
                got.append([(stage.at[t, pl.ds(at, size)], out_ref.at[unit, whose, pl.ds(row, size), pl.ds(pl.multiple_of(t * WIDE, WIDE), WIDE)],
                             o_sem.at[t, n])])
            else:
                token = pl.multiple_of(_flips(chip, unit) * 256 + whose * 128 + row, HALF)
                got.append([(stage.at[t, :, pl.ds(at, size)], o.at[:, pl.ds(token, size)], o_sem.at[t, n]) for o in outs])
            at += size
        return got

    def held_load(i):
        t, kc = i // steps, i % steps
        if gated:
            src = w_refs[0].at[pl.ds(kc * DEPTH, DEPTH), pl.ds(t * WIDE, WIDE)]
        else:
            src = w_refs[t].at[pl.ds(kc * DEPTH, DEPTH)]
        return pltpu.make_async_copy(src, held.at[i], w_sem.at[i])

    def part_load(i):
        t, kc = lax.div(i, steps), lax.rem(i, steps)
        return pltpu.make_async_copy(
            w_refs[1].at[pl.ds(pl.multiple_of(kc * DEPTH, DEPTH), DEPTH), pl.ds(pl.multiple_of(t * WIDE, WIDE), WIDE)],
            part.at[lax.rem(i, 4)], p_sem.at[lax.rem(i, 4)])

    for c in loads(0, True):
        c.start()
    for i in range(count):
        held_load(i).start()
        if gated and i < 3:
            part_load(i).start()
    _greet((near[X], near[Y], near[Z], sibling))
    cross[0, 0].start()
    for h in range(2):
        for n in range(3):
            first[h, n].start()
    cross[0, 0].wait_recv()
    for c in loads(0, False):
        c.start()

    for b, pieces in enumerate(blocks):
        size = sum(p[3] for p in pieces)
        slot = b % 2
        for c in loads(b, True) + loads(b, False):
            c.wait()

        def step(i, _, b=b, size=size, slot=slot, pieces=pieces):
            t, kc = lax.div(i, steps), lax.rem(i, steps)
            if b == 0:
                pltpu.make_async_copy(held.at[i], held.at[i], w_sem.at[i]).wait()
            left = lhs[slot, 0:size, pl.ds(pl.multiple_of(kc * DEPTH, DEPTH), DEPTH)]
            @pl.when(kc == 0)
            def _():
                total[...] = jnp.zeros_like(total)
            total[0, 0:size] += jnp.dot(left, held[i], preferred_element_type=jnp.float32)
            if gated:
                part_load(i).wait()
                more = i + 3 < count if b == len(blocks) - 1 else None
                def ahead():
                    part_load(lax.rem(i + 3, count)).start()
                ahead() if more is None else pl.when(more)(ahead)
                total[1, 0:size] += jnp.dot(left, part[lax.rem(i, 4)], preferred_element_type=jnp.float32)

            if b + 1 < len(blocks):
                @pl.when(i == count // 2 - 1)
                def _():
                    for c in arrivals(b + 1):
                        c.wait_recv()
                    for c in onward(b + 1):
                        c.start()
                    for n in range(3):
                        cross[b + 1, n].start()
                    for c in loads(b + 1, True):
                        c.start()

                @pl.when(i == count - 3)
                def _():
                    for n in range(3):
                        cross[b + 1, n].wait_recv()
                    for c in loads(b + 1, False):
                        c.start()

            @pl.when(kc == steps - 1)
            def _():
                if b > 0:
                    for group in stores(b - 1, t):
                        pltpu.make_async_copy(*group[0]).wait()
                if gated:
                    gate, up = total[0, 0:size], total[1, 0:size]
                    stage[t, 0:size] = (jax.nn.silu(gate) * up).astype(jnp.bfloat16)
                    for group in stores(b, t):
                        pltpu.make_async_copy(*group[0]).start()
                else:
                    @pl.when(t < 2)
                    def _():
                        at = 0
                        for unit, m, row, n in pieces:
                            token = pl.multiple_of(_flips(chip, unit) * 256 + (core if m else 1 - core) * 128 + row, HALF)
                            cos, sin = cos_ref[pl.ds(token, n)], sin_ref[pl.ds(token, n)]
                            for head in range(WIDE // HEAD):
                                flat = total[0, at : at + n, head * HEAD : (head + 1) * HEAD].astype(jnp.bfloat16).astype(jnp.float32)
                                stage[t, head, at : at + n] = (flat * cos + pltpu.roll(flat, HEAD // 2, 1) * sin).astype(jnp.bfloat16)
                            at += n

                    @pl.when(t == 2)
                    def _():
                        for head in range(WIDE // HEAD):
                            stage[t, head, 0:size] = total[0, 0:size, head * HEAD : (head + 1) * HEAD].astype(jnp.bfloat16)

                    for w in range(3):
                        @pl.when(t == w)
                        def _(w=w):
                            for group in stores(b, t):
                                pltpu.make_async_copy(*group[w]).start()

        lax.fori_loop(0, count, step, None)

    for t in range(tiles):
        for group in stores(len(blocks) - 1, t):
            pltpu.make_async_copy(*group[0]).wait()
    for c in [*first.values(), *second.values(), *third.values(), *cross.values()]:
        c.wait_send()


def fetched_qkv(a, wq, wk, wv, cos, sin):
    rows, depth = a.shape
    wide = wq.shape[1]
    tokens = 16 * rows
    hbm, vmem = pl.BlockSpec(memory_space=pl.ANY), pl.BlockSpec(memory_space=pltpu.VMEM)
    each = jax.ShapeDtypeStruct((wide // HEAD, tokens, HEAD), jnp.bfloat16)
    q, k, v, _ = pl.pallas_call(
        functools.partial(_gather_matmul, False),
        out_shape=[each, each, each, jax.ShapeDtypeStruct((8, 2, rows, depth), jnp.bfloat16)],
        in_specs=[hbm, hbm, hbm, hbm, vmem, vmem],
        out_specs=[hbm] * 4,
        scratch_shapes=[
            pltpu.VMEM((12, DEPTH, WIDE), jnp.bfloat16), pltpu.VMEM((2, 6 * HALF, depth), jnp.bfloat16), pltpu.VMEM((1, 6 * HALF, WIDE), jnp.float32),
            pltpu.VMEM((3, WIDE // HEAD, 6 * HALF, HEAD), jnp.bfloat16),
            pltpu.SemaphoreType.DMA((12,)), pltpu.SemaphoreType.DMA((2, 6)), pltpu.SemaphoreType.DMA((3, 6)),
            pltpu.SemaphoreType.DMA((15,)), pltpu.SemaphoreType.DMA((15,)), pltpu.SemaphoreType.DMA((16,)), pltpu.SemaphoreType.DMA((16,)),
        ],
        compiler_params=pltpu.CompilerParams(collective_id=0, has_side_effects=True, vmem_limit_bytes=KERNEL_VMEM),
        cost_estimate=pl.CostEstimate(flops=2 * tokens * depth * 3 * wide, transcendentals=0, bytes_accessed=2 * depth * (3 * wide + 2 * tokens)),
    )(a, wq, wk, wv, cos, sin)
    return q, k, v


def fetched_hidden(a, w_gate, w_up):
    rows, depth = a.shape
    wide = w_gate.shape[1]
    tokens = 16 * rows
    hbm = pl.BlockSpec(memory_space=pl.ANY)
    hidden, _ = pl.pallas_call(
        functools.partial(_gather_matmul, True),
        out_shape=[jax.ShapeDtypeStruct((8, 2, rows, wide), jnp.bfloat16), jax.ShapeDtypeStruct((8, 2, rows, depth), jnp.bfloat16)],
        in_specs=[hbm] * 3,
        out_specs=[hbm] * 2,
        scratch_shapes=[
            pltpu.VMEM((12, DEPTH, WIDE), jnp.bfloat16), pltpu.VMEM((4, DEPTH, WIDE), jnp.bfloat16),
            pltpu.VMEM((2, 6 * HALF, depth), jnp.bfloat16), pltpu.VMEM((2, 6 * HALF, WIDE), jnp.float32), pltpu.VMEM((3, 6 * HALF, WIDE), jnp.bfloat16),
            pltpu.SemaphoreType.DMA((12,)), pltpu.SemaphoreType.DMA((4,)), pltpu.SemaphoreType.DMA((2, 6)), pltpu.SemaphoreType.DMA((3, 6)),
            pltpu.SemaphoreType.DMA((15,)), pltpu.SemaphoreType.DMA((15,)), pltpu.SemaphoreType.DMA((16,)), pltpu.SemaphoreType.DMA((16,)),
        ],
        compiler_params=pltpu.CompilerParams(collective_id=1, has_side_effects=True, vmem_limit_bytes=KERNEL_VMEM),
        cost_estimate=pl.CostEstimate(flops=4 * tokens * depth * wide, transcendentals=tokens * wide, bytes_accessed=4 * depth * (wide + tokens)),
    )(a, w_gate, w_up)
    return hidden


IN = {X | Y: Y, Y | Z: Z, Z | X: X, X: X, Y: Y, Z: Z}
TAKES = {X: X | Y, Y: Y | Z, Z: Z | X}
FAR = (7, X | Y, Y | Z, Z | X)
NEAR = (X, Y, Z)
LIVE = 5
STEPS = ((7, 0), (7, 1), *((u, 0) for u in FAR[1:]), *((u, 1) for u in FAR[1:]), *((u, 0) for u in NEAR), *((u, 1) for u in NEAR), (0, 0), (0, 1))


def _matmul_scatter(heads, a_ref, w_ref, x_ref, out_ref, last_ref, w, lhs, own, mate, dsend, isend, inc, tin,
                    w_sem, l_sem, t_sem, send, recv, csend, crecv, credit, o_sem):
    chip, core, near, sibling = _places()
    half = w_ref.shape[1] // 2
    tiles = half // WIDE

    def w_load(t):
        cols = pl.ds(t * WIDE, WIDE) if isinstance(t, int) else pl.ds(pl.multiple_of(t * WIDE, WIDE), WIDE)
        return pltpu.make_async_copy(w_ref.at[:, cols], w.at[:, cols], w_sem.at[t])

    def lhs_loads(n):
        unit, got = STEPS[n][0], []
        for i, whose in enumerate((core, 1 - core)):
            to = pl.ds(i * 128, 128)
            if heads:
                token = pl.multiple_of(_flips(chip, unit) * 256 + whose * 128, 128)
                for head in range(heads):
                    got.append(pltpu.make_async_copy(a_ref.at[head, pl.ds(token, 128)], lhs.at[n % 2, to, pl.ds(head * HEAD, HEAD)],
                                                     l_sem.at[n % 2, i * heads + head]))
            else:
                got.append(pltpu.make_async_copy(a_ref.at[unit, whose], lhs.at[n % 2, to], l_sem.at[n % 2, i]))
        return got

    def across(n):
        return pltpu.make_async_remote_copy(dsend.at[n % 2], mate.at[n % LIVE], csend.at[n], crecv.at[n], device_id={"tp": sibling}, device_id_type=MESH)

    def place(unit):
        return FAR.index(unit) if unit in FAR else NEAR.index(unit)

    def hop(unit, h, p):
        at, size, _, axis = THIRDS[p]
        axis = axis if unit == 7 else IN[unit]
        to = inc.at[FAR.index(unit)] if unit in FAR else last_ref.at[NEAR.index(unit)]
        return pltpu.make_async_remote_copy(isend.at[place(unit), h, pl.ds(at, size)], to.at[h, pl.ds(at, size)], send.at[unit, h, p],
                                            recv.at[unit, h, p], device_id={"tp": near[axis]}, device_id_type=MESH)

    done, met = {}, set()

    def compute(n):
        unit, h = STEPS[n]
        if n >= LIVE and len(done[n - LIVE]) < 3:
            raise ValueError
        for c in lhs_loads(n):
            c.wait()
        if n + 1 < len(STEPS):
            for c in lhs_loads(n + 1):
                c.start()
        if n >= 2:
            across(n - 2).wait_send()

        def tile(t, _):
            cols = pl.ds(pl.multiple_of(t * WIDE, WIDE), WIDE)
            from_w = pl.ds(pl.multiple_of(h * half + t * WIDE, WIDE), WIDE)
            if n < 2:
                w_load(h * tiles + t).wait()
            got = jnp.dot(lhs[n % 2], w[:, from_w], preferred_element_type=jnp.float32)
            own[n % LIVE, :, cols] = got[:128]
            dsend[n % 2, :, cols] = got[128:].astype(jnp.bfloat16)

        lax.fori_loop(0, tiles, tile, None)
        if n >= LIVE:
            pl.semaphore_wait(credit.at[n % LIVE], 1)
        across(n).start()

    def finish(n, p):
        unit, h = STEPS[n]
        at, size, third, _ = THIRDS[p]
        if n not in met:
            met.add(n)
            across(n).wait_recv()
        here = pl.ds(at, size)
        source = TAKES.get(unit, 7 if third == unit else None)
        if source is not None:
            hop(source, h, p).wait_recv()
        if unit in NEAR:
            hop(FAR[NEAR.index(unit)], h, p).wait_send()

        def tile(t, _):
            cols = pl.ds(pl.multiple_of(t * WIDE, WIDE), WIDE)
            got = own[n % LIVE, here, cols] + mate[n % LIVE, here, cols].astype(jnp.float32)
            if source is not None:
                got += inc[FAR.index(source), h, here, cols].astype(jnp.float32)
            isend[place(unit), h, here, cols] = got.astype(jnp.bfloat16)

        lax.fori_loop(0, tiles, tile, None)
        hop(unit, h, p).start()
        over(n, p)

    def over(n, p):
        done.setdefault(n, set()).add(p)
        if len(done[n]) == 3 and n + LIVE < len(STEPS):
            pl.semaphore_signal(credit.at[n % LIVE], inc=1, device_id={"tp": sibling}, device_id_type=MESH)

    def last_loads(h, p):
        at, size, _, _ = THIRDS[p]
        to, here = (h * 3 + p) % 2, pl.ds(at, size)
        got = [pltpu.make_async_copy(last_ref.at[i, h, here], tin.at[to, i, 0:size], t_sem.at[to, i]) for i in range(3)]
        return got + [pltpu.make_async_copy(x_ref.at[here, pl.ds(h * half, half)], tin.at[to, 3, 0:size], t_sem.at[to, 3])]

    def fetch_last(h, p):
        for unit in NEAR:
            hop(unit, h, p).wait_recv()
        for c in last_loads(h, p):
            c.start()

    def put(h, p):
        at, size, _, _ = THIRDS[p]
        return pltpu.make_async_copy(isend.at[3, h, pl.ds(at, size)], out_ref.at[pl.ds(at, size), pl.ds(h * half, half)], o_sem.at[h, p])

    def finish_last(h, p):
        at, size, _, _ = THIRDS[p]
        n, here = STEPS.index((0, h)), pl.ds(at, size)
        if n not in met:
            met.add(n)
            across(n).wait_recv()
        hop(FAR[3], h, p).wait_send()
        for c in last_loads(h, p):
            c.wait()

        def tile(t, _):
            cols = pl.ds(pl.multiple_of(t * WIDE, WIDE), WIDE)
            got = own[n % LIVE, here, cols] + mate[n % LIVE, here, cols].astype(jnp.float32)
            for i in range(4):
                got += tin[(h * 3 + p) % 2, i, 0:size, cols].astype(jnp.float32)
            isend[3, h, here, cols] = got.astype(jnp.bfloat16)

        lax.fori_loop(0, tiles, tile, None)
        put(h, p).start()

    for c in lhs_loads(0):
        c.start()
    for t in range(2 * tiles):
        w_load(t).start()
    _greet((near[X], near[Y], near[Z], sibling))

    for n, sums in (
        (0, ()), (1, ((0, 0), (0, 1), (0, 2))), (2, ((1, 0), (1, 1), (1, 2))), (3, ((2, 1), (2, 2))), (4, ((3, 0), (3, 2))),
        (5, ((4, 0), (4, 1), (2, 0))), (6, ((5, 1), (5, 2), (3, 1))), (7, ((6, 0), (6, 2), (4, 2))),
        (8, ((7, 0), (7, 1), (5, 0), (6, 1), (7, 2))), (9, ()), (10, ()), (11, ()),
        (12, [(8 + i, p) for p in range(3) for i in range(3)]), (13, ()), (14, [(11 + i, p) for p in range(3) for i in range(3)]), (15, ()),
    ):
        compute(n)
        for sum in sums:
            finish(*sum)
    ends = [(h, p) for h in range(2) for p in range(3)]
    fetch_last(*ends[0])
    for i, end in enumerate(ends):
        if i + 1 < len(ends):
            fetch_last(*ends[i + 1])
        finish_last(*end)
    for end in ends:
        put(*end).wait()
        for unit in NEAR:
            hop(unit, *end).wait_send()
    for n in (14, 15):
        across(n).wait_send()


def summed(x, a, w, number):
    rows, columns = x.shape
    depth, half = w.shape[0], columns // 2
    heads = a.shape[0] if a.ndim == 3 else 0
    hbm = pl.BlockSpec(memory_space=pl.ANY)
    dma = pltpu.SemaphoreType.DMA
    low = jnp.bfloat16
    out, _ = pl.pallas_call(
        functools.partial(_matmul_scatter, heads),
        out_shape=[jax.ShapeDtypeStruct((rows, columns), low), jax.ShapeDtypeStruct((3, 2, rows, half), low)],
        in_specs=[hbm] * 3,
        out_specs=[hbm] * 2,
        scratch_shapes=[
            pltpu.VMEM((depth, columns), low), pltpu.VMEM((2, 2 * rows, depth), low), pltpu.VMEM((LIVE, rows, half), jnp.float32),
            pltpu.VMEM((LIVE, rows, half), low), pltpu.VMEM((2, rows, half), low), pltpu.VMEM((4, 2, rows, half), low),
            pltpu.VMEM((4, 2, rows, half), low), pltpu.VMEM((2, 4, 48, half), low),
            dma((columns // WIDE,)), dma((2, 2 * max(heads, 1))), dma((2, 4)), dma((8, 2, 3)), dma((8, 2, 3)), dma((16,)), dma((16,)),
            pltpu.SemaphoreType.REGULAR((LIVE,)), dma((2, 3)),
        ],
        compiler_params=pltpu.CompilerParams(collective_id=number, has_side_effects=True, vmem_limit_bytes=KERNEL_VMEM),
        cost_estimate=pl.CostEstimate(flops=32 * rows * depth * columns, transcendentals=0, bytes_accessed=2 * columns * (depth + 32 * rows)),
    )(a, w, x)
    return out


def solution(mesh):
    def step(x, gain_a, wq, wk, wv, wo, gain_m, w_gate, w_up, w_down):
        tokens = 16 * x.shape[0]
        half = HEAD // 2
        angle = jnp.arange(tokens).astype(jnp.float32)[:, None] * THETA ** (-jnp.arange(half, dtype=jnp.float32) / half)
        cos, sin = jnp.cos(angle), jnp.sin(angle)
        q, k, v = fetched_qkv(normed(x, gain_a), wq, wk, wv, jnp.concatenate([cos, cos], -1), jnp.concatenate([-sin, sin], -1))
        seen = attend(q, k, v)
        h = summed(x, seen, wo, 2)
        return summed(h, fetched_hidden(normed(h, gain_m), w_gate, w_up), w_down, 3)

    tokens, columns, rows_of = P(("dp", "tp"), None), P(None, "tp"), P("tp", None)
    return jax.shard_map(
        step,
        mesh=mesh,
        in_specs=(tokens, P(None), columns, columns, columns, rows_of, P(None), columns, columns, rows_of),
        out_specs=tokens,
        check_vma=False,
    )
```

```python
import functools

import jax
import jax.numpy as jnp
import numpy as np
from jax import lax
from jax.experimental import pallas as pl
from jax.experimental.pallas import tpu as pltpu

NEG = -1e30
HIDDEN = 2 * NEG
LOG2E = 1.4426950408889634


def _dot(a, b, ca, cb):
    return lax.dot_general(a, b, (((ca,), (cb,)), ((), ())), preferred_element_type=jnp.float32)


from jax.sharding import PartitionSpec as P

HEAD = 128
THETA = 10000
MESH = pl.DeviceIdType.MESH
KERNEL_VMEM = 66_000_000
X, Y, Z = 4, 2, 1
OUT = ((X, X | Y, Y), (Y, Y | Z, Z), (Z, Z | X, X))
THIRDS = ((0, 48, X | Y, Z), (48, 48, Y | Z, X), (96, 32, Z | X, Y))
WIDE = 512


def _flip(n, bit):
    return n + bit - 2 * bit * lax.rem(lax.div(n, bit), 2)


def _flips(n, bits):
    for bit in (4, 2, 1):
        if bits & bit:
            n = _flip(n, bit)
    return n


def _places():
    me = lax.axis_index("tp")
    chip, core = lax.div(me, 2), lax.rem(me, 2)
    return chip, core, {axis: _flip(me, 2 * axis) for axis in (X, Y, Z)}, _flip(me, 1)


def _greet(partners):
    barrier = pltpu.get_barrier_semaphore()
    for partner in partners:
        pl.semaphore_signal(barrier, inc=1, device_id={"tp": partner}, device_id_type=MESH)
    pl.semaphore_wait(barrier, len(partners))


def _normed(t_ref, gain, first, size, *to):
    def some(i, _):
        here = pl.ds(pl.multiple_of(i * 16, 16), 16)
        wide = t_ref[here].astype(jnp.float32)
        scale = lax.rsqrt(jnp.mean(wide * wide, -1, keepdims=True) + 1e-6)
        got = (wide * scale * gain).astype(jnp.bfloat16)
        for ref in to:
            ref[here] = got

    lax.fori_loop(first // 16, (first + size) // 16, some, None)


def _gather_matmul(gated, t_ref, gain_ref, *refs):
    (w_refs, refs) = (refs[:2], refs[2:]) if gated else (refs[:3], refs[3:])
    if not gated:
        turn_ref, refs = refs[0], refs[1:]
    (outs, refs) = (refs[:1], refs[1:]) if gated else (refs[:3], refs[3:])
    all_ref, held, raw, mine, lhs, total, stage, w_sem, p_sem, l_sem, o_sem, send, recv, csend, crecv, r_sem = refs
    chip, core, near, sibling = _places()
    ways = 2 if gated else 1
    tiles = 3

    def hop(i, src, dst, axis):
        return pltpu.make_async_remote_copy(src, dst, send.at[i], recv.at[i], device_id={"tp": near[axis]}, device_id_type=MESH)

    def across(i, src, dst):
        return pltpu.make_async_remote_copy(src, dst, csend.at[i], crecv.at[i], device_id={"tp": sibling}, device_id_type=MESH)

    def rows(unit, whose, at, n):
        return all_ref.at[unit, whose, pl.ds(at, n)]

    hops, cross = {g: [] for g in range(1, 8)}, {g: [] for g in range(1, 8)}
    blocks = [[(0, m, 0, 128) for m in (True, False)]]
    for leg in range(2):
        for p, (at, size, _, _) in enumerate(THIRDS):
            g = 1 + leg * 3 + p
            for n, (one, two, axis) in enumerate(OUT):
                src, unit, way = (rows(one, core, at, size), two, axis) if leg else (mine.at[pl.ds(at, size)], one, one)
                hops[g].append(hop((g - 1) * 3 + n, src, rows(unit, core, at, size), way))
                cross[g].append(across(g * 3 + n, rows(unit, core, at, size), rows(unit, core, at, size)))
            blocks.append([(way[leg], m, at, size) for m in (True, False) for way in OUT])
    for n, (at, size, source, axis) in enumerate(THIRDS):
        hops[7].append(hop(18 + n, rows(source, core, at, size), rows(7, core, at, size), axis))
        cross[7].append(across(21 + n, rows(7, core, at, size), rows(7, core, at, size)))
    blocks += [[(7, m, 0, 128)] for m in (True, False)]
    own = across(0, mine, rows(0, core, 0, 128))
    last = len(blocks) - 1
    early, late = (2, 4) if gated else (2, 2)

    def loads(b, m):
        at, got = 0, []
        for n, (unit, whose, row, size) in enumerate(blocks[b]):
            if whose == m and not (m and unit == 0):
                got.append(pltpu.make_async_copy(rows(unit, core if m else 1 - core, row, size), lhs.at[b % 2, pl.ds(at, size)], l_sem.at[b % 2, n]))
            at += size
        return got

    def arrive(b):
        if b == last:
            return
        for c in hops[b]:
            c.wait_recv()
        for c in hops[b + 3] if b < 4 else hops[7][b - 4 : b - 3]:
            c.start()
        for c in cross[b]:
            c.start()
        for c in loads(b, True):
            c.start()

    def settle(b):
        if b == last - 1:
            return
        for c in cross[min(b, 7)]:
            c.wait_recv()
        for c in loads(b, False):
            c.start()

    def stores(b, t, out):
        at, got = 0, []
        for n, (unit, m, row, size) in enumerate(blocks[b]):
            whose = core if m else 1 - core
            if gated:
                to = out.at[unit, whose, pl.ds(row, size), pl.ds(pl.multiple_of(t * WIDE, WIDE), WIDE)]
                got.append(pltpu.make_async_copy(stage.at[t, pl.ds(at, size)], to, o_sem.at[t, n]))
            else:
                token = pl.multiple_of((_flips(chip, unit) * 2 + whose) * 128 + row, 16)
                got.append(pltpu.make_async_copy(stage.at[t, :, pl.ds(at, size)], out.at[:, pl.ds(token, size)], o_sem.at[t, n]))
            at += size
        return got

    def held_load(t):
        return pltpu.make_async_copy(w_refs[0].at[:, pl.ds(t * WIDE, WIDE)] if gated else w_refs[t], held.at[t], w_sem.at[t])

    def part_load(n):
        to = lax.rem(n, 2)
        return pltpu.make_async_copy(w_refs[1].at[:, pl.ds(pl.multiple_of(lax.rem(n, tiles) * WIDE, WIDE), WIDE)], held.at[tiles + to], p_sem.at[to])

    first = pltpu.make_async_copy(t_ref, raw, r_sem)
    first.start()
    partners = (near[X], near[Y], near[Z], sibling)
    barrier = pltpu.get_barrier_semaphore()
    for partner in partners:
        pl.semaphore_signal(barrier, inc=1, device_id={"tp": partner}, device_id_type=MESH)
    first.wait()
    for t in range(tiles):
        held_load(t).start()
        if gated and t < 2:
            part_load(t).start()
    for g, (at, size, _, _) in enumerate(THIRDS, 1):
        _normed(raw, gain_ref[1 if gated else 0 : 2 if gated else 1].astype(jnp.float32), at, size, mine, lhs.at[0])
        if g == 1:
            pl.semaphore_wait(barrier, len(partners))
        for c in hops[g]:
            c.start()
    own.start()
    own.wait_recv()
    for c in loads(0, False):
        c.start()

    for b, pieces in enumerate(blocks):
        size = sum(p[3] for p in pieces)
        for c in loads(b, True) + loads(b, False):
            c.wait()

        def step(j, _, b=b, size=size, pieces=pieces):
            t, way = lax.div(j, ways), lax.rem(j, ways)
            n = b * tiles + t
            if b == 0:
                @pl.when(way == 0)
                def _():
                    pltpu.make_async_copy(held.at[t], held.at[t], w_sem.at[t]).wait()
            if gated:
                @pl.when(way == 1)
                def _():
                    part_load(n).wait()
            which = (1 - way) * t + way * (tiles + lax.rem(n, 2))
            total[way, 0:size] = jnp.dot(lhs[b % 2, 0:size], held[which], preferred_element_type=jnp.float32)
            if gated:
                @pl.when((way == 1) & (n + 2 < len(blocks) * tiles))
                def _():
                    part_load(n + 2).start()

            @pl.when(way == ways - 1)
            def _():
                if b > 0:
                    for c in stores(b - 1, t, outs[0]):
                        c.wait()
                if gated:
                    stage[t, 0:size] = (jax.nn.silu(total[0, 0:size]) * total[1, 0:size]).astype(jnp.bfloat16)
                    for c in stores(b, t, outs[0]):
                        c.start()
                else:
                    @pl.when(t < 2)
                    def _():
                        at = 0
                        for unit, m, row, n in pieces:
                            shard = _flips(chip, unit) * 2 + (core if m else 1 - core)
                            cos, sin = (turn_ref[i, row : row + n] for i in range(2))
                            cos_far, sin_far = (turn_ref[i, pl.ds(128 + shard, 1)] for i in range(2))
                            cos, sin = cos_far * cos - sin_far * sin, sin_far * cos + cos_far * sin
                            for head in range(WIDE // HEAD):
                                flat = total[0, at : at + n, head * HEAD : (head + 1) * HEAD].astype(jnp.bfloat16).astype(jnp.float32)
                                stage[t, head, at : at + n] = (flat * cos + pltpu.roll(flat, HEAD // 2, 1) * sin).astype(jnp.bfloat16)
                            at += n

                    @pl.when(t == 2)
                    def _():
                        for head in range(WIDE // HEAD):
                            stage[t, head, 0:size] = total[0, 0:size, head * HEAD : (head + 1) * HEAD].astype(jnp.bfloat16)

                    for w in range(3):
                        @pl.when(t == w)
                        def _(w=w):
                            for c in stores(b, t, outs[w]):
                                c.start()

            if b < last:
                @pl.when(j == early)
                def _():
                    arrive(b + 1)

                @pl.when(j == late)
                def _():
                    settle(b + 1)

        lax.fori_loop(0, ways * tiles, step, None)

    for t in range(3):
        for c in stores(last, t, outs[0]):
            c.wait()
    own.wait_send()
    for g in hops:
        for c in hops[g] + cross[g]:
            c.wait_send()


def fetched(t, gains, weights, outs, number, turn=None):
    rows, columns = t.shape
    gated = turn is None
    hbm, vmem = pl.BlockSpec(memory_space=pl.ANY), pl.BlockSpec(memory_space=pltpu.VMEM)
    dma, low = pltpu.SemaphoreType.DMA, jnp.bfloat16
    most = 6 * 48
    flops = 32 * rows * columns * sum(w.shape[1] for w in weights)
    return pl.pallas_call(
        functools.partial(_gather_matmul, gated),
        out_shape=[*(jax.ShapeDtypeStruct(shape, low) for shape in outs), jax.ShapeDtypeStruct((8, 2, rows, columns), low)],
        in_specs=[hbm, vmem] + [hbm] * len(weights) + [vmem] * (not gated),
        out_specs=[hbm] * (len(outs) + 1),
        scratch_shapes=[
            pltpu.VMEM((3 + 2 * gated, columns, WIDE), low), pltpu.VMEM((rows, columns), low), pltpu.VMEM((rows, columns), low),
            pltpu.VMEM((2, most, columns), low), pltpu.VMEM((1 + gated, most, WIDE), jnp.float32),
            pltpu.VMEM((3, most, WIDE) if gated else (3, WIDE // HEAD, most, HEAD), low),
            dma((3,)), dma((2,)), dma((2, 6)), dma((3, 6)), dma((21,)), dma((21,)), dma((24,)), dma((24,)), dma(()),
        ],
        compiler_params=pltpu.CompilerParams(collective_id=number, has_side_effects=True, vmem_limit_bytes=KERNEL_VMEM),
        cost_estimate=pl.CostEstimate(flops=flops, transcendentals=0, bytes_accessed=flops // 512),
    )(t, gains, *weights, *(() if gated else (turn,)))[: len(outs)]


IN = {X | Y: Y, Y | Z: Z, Z | X: X, X: X, Y: Y, Z: Z}
TAKES = {X: X | Y, Y: Y | Z, Z: Z | X}
FAR = (7, X | Y, Y | Z, Z | X)
NEAR = (X, Y, Z)
LIVE = 5
STEPS = ((7, 0), (7, 1), *((u, 0) for u in FAR[1:]), *((u, 1) for u in FAR[1:]), *((u, 0) for u in NEAR), *((u, 1) for u in NEAR), (0, 0), (0, 1))


def _attend(q, k, v, first, put, top_s, mix_s, gap_s, scale):
    bk = gap_s.shape[0]
    e = scale * LOG2E
    ones = jnp.ones((8, bk), q.dtype)
    heads = range(q.shape[0])

    top_s[...] = jnp.full(top_s.shape, NEG, jnp.float32)
    mix_s[...] = jnp.zeros(mix_s.shape, jnp.float32)

    def block(j, _):
        here = pl.ds(pl.multiple_of(j * bk, bk), bk)
        seen = gap_s[...] >= j * bk - first
        scores = [_dot(k[i, here], q[i, pl.ds(first, bk)], 1, 1) for i in heads]
        weights, keeps = [], []
        for i, s in zip(heads, scores):
            s = jnp.where(seen, s, HIDDEN)
            old = top_s[i : i + 1]
            top = jnp.maximum(old, s.max(axis=0, keepdims=True))
            top_s[i : i + 1] = top
            weights.append(jnp.exp2((s - top) * e).astype(q.dtype))
            keeps.append(jnp.exp2((old - top) * e))
        for i, p, keep in zip(heads, weights, keeps):
            mix_s[i] = mix_s[i] * keep + _dot(jnp.concatenate([v[i, here].T, ones], axis=0), p, 1, 0)

    lax.fori_loop(0, lax.div(first, bk) + 1, block, None)
    for i in heads:
        put(i, (mix_s[i, :HEAD] * (1 / mix_s[i, HEAD : HEAD + 1])).T.astype(q.dtype))


def _matmul_scatter(heads, *refs):
    a_refs, refs = (refs[:3], refs[3:]) if heads else (refs[:1], refs[1:])
    (w_ref, x_ref, out_ref, last_ref, w, lhs, own, mate, dsend, isend, inc, tin, w_sem, l_sem, t_sem, send, recv, csend, crecv, credit, o_sem) = refs[:21]
    if heads:
        *qkv, top_s, mix_s, gap_s = refs[21:]
    chip, core, near, sibling = _places()
    half = w_ref.shape[1] // 2
    tiles = half // WIDE

    def w_load(t):
        cols = pl.ds(t * WIDE, WIDE) if isinstance(t, int) else pl.ds(pl.multiple_of(t * WIDE, WIDE), WIDE)
        return pltpu.make_async_copy(w_ref.at[:, cols], w.at[:, cols], w_sem.at[t])

    def lhs_loads(n):
        if heads:
            return [pltpu.make_async_copy(a, b, l_sem.at[0, i]) for i, (a, b) in enumerate(zip(a_refs, qkv))] if n == 0 else []
        return [pltpu.make_async_copy(a_refs[0].at[STEPS[n][0], whose], lhs.at[n % 2, pl.ds(i * 128, 128)], l_sem.at[n % 2, i])
                for i, whose in enumerate((core, 1 - core))]

    def attended(unit):
        def put(head, got):
            cols = pl.ds(head * HEAD, HEAD)
            lhs[unit, pl.ds(pl.multiple_of(core * 128, 128), 128), cols] = got[:128]
            lhs[unit, pl.ds(pl.multiple_of(128 - core * 128, 128), 128), cols] = got[128:]

        _attend(*qkv, pl.multiple_of(_flips(chip, unit) * 256, 256), put, top_s, mix_s, gap_s, HEAD**-0.5)

    def across(n):
        return pltpu.make_async_remote_copy(dsend.at[n % 2], mate.at[n % LIVE], csend.at[n], crecv.at[n], device_id={"tp": sibling}, device_id_type=MESH)

    def place(unit):
        return FAR.index(unit) if unit in FAR else NEAR.index(unit)

    def hop(unit, h, p):
        at, size, _, axis = THIRDS[p]
        axis = axis if unit == 7 else IN[unit]
        to = inc.at[FAR.index(unit)] if unit in FAR else last_ref.at[NEAR.index(unit)]
        return pltpu.make_async_remote_copy(isend.at[place(unit), h, pl.ds(at, size)], to.at[h, pl.ds(at, size)], send.at[unit, h, p],
                                            recv.at[unit, h, p], device_id={"tp": near[axis]}, device_id_type=MESH)

    done, met = {}, set()

    def compute(n):
        unit, h = STEPS[n]
        if n >= LIVE and len(done[n - LIVE]) < 3:
            raise ValueError
        for c in lhs_loads(n):
            c.wait()
        if n + 1 < len(STEPS):
            for c in lhs_loads(n + 1):
                c.start()
        if heads and unit not in [u for u, _ in STEPS[:n]]:
            attended(unit)
        if n >= 2:
            across(n - 2).wait_send()

        def tile(t, _):
            cols = pl.ds(pl.multiple_of(t * WIDE, WIDE), WIDE)
            from_w = pl.ds(pl.multiple_of(h * half + t * WIDE, WIDE), WIDE)
            if n < 2:
                w_load(h * tiles + t).wait()
            got = jnp.dot(lhs[unit if heads else n % 2], w[:, from_w], preferred_element_type=jnp.float32)
            own[n % LIVE, :, cols] = got[:128]
            dsend[n % 2, :, cols] = got[128:].astype(jnp.bfloat16)

        lax.fori_loop(0, tiles, tile, None)
        if n >= LIVE:
            pl.semaphore_wait(credit.at[n % LIVE], 1)
        across(n).start()

    def finish(n, p):
        unit, h = STEPS[n]
        at, size, third, _ = THIRDS[p]
        if n not in met:
            met.add(n)
            across(n).wait_recv()
        here = pl.ds(at, size)
        source = TAKES.get(unit, 7 if third == unit else None)
        if source is not None:
            hop(source, h, p).wait_recv()
        if unit in NEAR:
            hop(FAR[NEAR.index(unit)], h, p).wait_send()

        def tile(t, _):
            cols = pl.ds(pl.multiple_of(t * WIDE, WIDE), WIDE)
            got = own[n % LIVE, here, cols] + mate[n % LIVE, here, cols].astype(jnp.float32)
            if source is not None:
                got += inc[FAR.index(source), h, here, cols].astype(jnp.float32)
            isend[place(unit), h, here, cols] = got.astype(jnp.bfloat16)

        lax.fori_loop(0, tiles, tile, None)
        hop(unit, h, p).start()
        over(n, p)

    def over(n, p):
        done.setdefault(n, set()).add(p)
        if len(done[n]) == 3 and n + LIVE < len(STEPS):
            pl.semaphore_signal(credit.at[n % LIVE], inc=1, device_id={"tp": sibling}, device_id_type=MESH)

    def last_loads(h, p):
        at, size, _, _ = THIRDS[p]
        to, here = (h * 3 + p) % 2, pl.ds(at, size)
        got = [pltpu.make_async_copy(last_ref.at[i, h, here], tin.at[to, i, 0:size], t_sem.at[to, i]) for i in range(3)]
        return got + [pltpu.make_async_copy(x_ref.at[here, pl.ds(h * half, half)], tin.at[to, 3, 0:size], t_sem.at[to, 3])]

    def fetch_last(h, p):
        for unit in NEAR:
            hop(unit, h, p).wait_recv()
        for c in last_loads(h, p):
            c.start()

    def put(h, p):
        at, size, _, _ = THIRDS[p]
        return pltpu.make_async_copy(isend.at[3, h, pl.ds(at, size)], out_ref.at[pl.ds(at, size), pl.ds(h * half, half)], o_sem.at[h, p])

    def finish_last(h, p):
        at, size, _, _ = THIRDS[p]
        n, here = STEPS.index((0, h)), pl.ds(at, size)
        if n not in met:
            met.add(n)
            across(n).wait_recv()
        hop(FAR[3], h, p).wait_send()
        for c in last_loads(h, p):
            c.wait()

        def tile(t, _):
            cols = pl.ds(pl.multiple_of(t * WIDE, WIDE), WIDE)
            got = own[n % LIVE, here, cols] + mate[n % LIVE, here, cols].astype(jnp.float32)
            for i in range(4):
                got += tin[(h * 3 + p) % 2, i, 0:size, cols].astype(jnp.float32)
            isend[3, h, here, cols] = got.astype(jnp.bfloat16)

        lax.fori_loop(0, tiles, tile, None)
        put(h, p).start()

    for c in lhs_loads(0):
        c.start()
    for t in range(2 * tiles):
        w_load(t).start()
    if heads:
        gap_s[...] = lax.broadcasted_iota(jnp.int32, gap_s.shape, 1) - lax.broadcasted_iota(jnp.int32, gap_s.shape, 0)
    _greet((near[X], near[Y], near[Z], sibling))

    for n, sums in (
        (0, ()), (1, ((0, 0), (0, 1), (0, 2))), (2, ((1, 0), (1, 1), (1, 2))), (3, ((2, 1), (2, 2))), (4, ((3, 0), (3, 2))),
        (5, ((4, 0), (4, 1), (2, 0))), (6, ((5, 1), (5, 2), (3, 1))), (7, ((6, 0), (6, 2), (4, 2))),
        (8, ((7, 0), (7, 1), (5, 0), (6, 1), (7, 2))), (9, ()), (10, ()), (11, ()),
        (12, [(8 + i, p) for p in range(3) for i in range(3)]), (13, ()), (14, [(11 + i, p) for p in range(3) for i in range(3)]), (15, ()),
    ):
        compute(n)
        for sum in sums:
            finish(*sum)
    ends = [(h, p) for h in range(2) for p in range(3)]
    fetch_last(*ends[0])
    for i, end in enumerate(ends):
        if i + 1 < len(ends):
            fetch_last(*ends[i + 1])
        finish_last(*end)
    for end in ends:
        put(*end).wait()
        for unit in NEAR:
            hop(unit, *end).wait_send()
    for n in (14, 15):
        across(n).wait_send()


def summed(x, a, w, number):
    rows, columns = x.shape
    depth, half = w.shape[0], columns // 2
    heads = len(a) == 3
    hbm = pl.BlockSpec(memory_space=pl.ANY)
    dma = pltpu.SemaphoreType.DMA
    low, wide = jnp.bfloat16, jnp.float32
    out, _ = pl.pallas_call(
        functools.partial(_matmul_scatter, heads),
        out_shape=[jax.ShapeDtypeStruct((rows, columns), low), jax.ShapeDtypeStruct((3, 2, rows, half), low)],
        in_specs=[hbm] * (len(a) + 2),
        out_specs=[hbm] * 2,
        scratch_shapes=[
            pltpu.VMEM((depth, columns), low), pltpu.VMEM((8 if heads else 2, 2 * rows, depth), low), pltpu.VMEM((LIVE, rows, half), wide),
            pltpu.VMEM((LIVE, rows, half), low), pltpu.VMEM((2, rows, half), low), pltpu.VMEM((4, 2, rows, half), low),
            pltpu.VMEM((4, 2, rows, half), low), pltpu.VMEM((2, 4, 48, half), low),
            dma((columns // WIDE,)), dma((2, 3)), dma((2, 4)), dma((8, 2, 3)), dma((8, 2, 3)), dma((16,)), dma((16,)),
            pltpu.SemaphoreType.REGULAR((LIVE,)), dma((2, 3)),
        ] + ([pltpu.VMEM(t.shape, low) for t in a] + [pltpu.VMEM((4, 256), wide), pltpu.VMEM((4, HEAD + 8, 256), wide), pltpu.VMEM((256, 256), jnp.int32)]
             if heads else []),
        compiler_params=pltpu.CompilerParams(collective_id=number, has_side_effects=True, vmem_limit_bytes=KERNEL_VMEM),
        cost_estimate=pl.CostEstimate(flops=32 * rows * depth * columns, transcendentals=0, bytes_accessed=2 * columns * (depth + 32 * rows)),
    )(*a, w, x)
    return out


def turns():
    place = np.concatenate([np.arange(128), 128 * np.arange(16)])
    angle = place[:, None] * float(THETA) ** (-np.arange(HEAD // 2) / (HEAD // 2))
    cos, sin = np.cos(angle), np.sin(angle)
    return np.stack([np.concatenate([cos, cos], -1), np.concatenate([-sin, sin], -1)]).astype(np.float32)


def solution(mesh):
    def step(x, gain_a, wq, wk, wv, wo, gain_m, w_gate, w_up, w_down):
        rows, wide = x.shape[0], wo.shape[0]
        gains = jnp.stack([gain_a, gain_m])
        qkv = fetched(x, gains, (wq, wk, wv), [(wide // HEAD, 16 * rows, HEAD)] * 3, 0, turns())
        h = summed(x, qkv, wo, 2)
        (hidden,) = fetched(h, gains, (w_gate, w_up), [(8, 2, rows, w_up.shape[1])], 1)
        return summed(h, (hidden,), w_down, 3)

    tokens, columns, rows_of = P(("dp", "tp"), None), P(None, "tp"), P("tp", None)
    return jax.shard_map(
        step,
        mesh=mesh,
        in_specs=(tokens, P(None), columns, columns, columns, rows_of, P(None), columns, columns, rows_of),
        out_specs=tokens,
        check_vma=False,
    )
```

```python
import functools

import jax
import jax.numpy as jnp
import numpy as np
from jax import lax
from jax.experimental import pallas as pl
from jax.experimental.pallas import tpu as pltpu

NEG = -1e30
HIDDEN = 2 * NEG
LOG2E = 1.4426950408889634


def _dot(a, b, ca, cb):
    return lax.dot_general(a, b, (((ca,), (cb,)), ((), ())), preferred_element_type=jnp.float32)


from jax.sharding import PartitionSpec as P

HEAD = 128
THETA = 10000
MESH = pl.DeviceIdType.MESH
KERNEL_VMEM = 66_000_000
X, Y, Z = 4, 2, 1
OUT = ((X, X | Y, Y), (Y, Y | Z, Z), (Z, Z | X, X))
THIRDS = ((0, 48, X | Y, Z), (48, 48, Y | Z, X), (96, 32, Z | X, Y))
WIDE = 512


def _flip(n, bit):
    return n + bit - 2 * bit * lax.rem(lax.div(n, bit), 2)


def _flips(n, bits):
    for bit in (4, 2, 1):
        if bits & bit:
            n = _flip(n, bit)
    return n


def _places():
    me = lax.axis_index("tp")
    chip, core = lax.div(me, 2), lax.rem(me, 2)
    return chip, core, {axis: _flip(me, 2 * axis) for axis in (X, Y, Z)}, _flip(me, 1)


def _greet(partners):
    barrier = pltpu.get_barrier_semaphore()
    for partner in partners:
        pl.semaphore_signal(barrier, inc=1, device_id={"tp": partner}, device_id_type=MESH)
    pl.semaphore_wait(barrier, len(partners))


def _normed(t_ref, gain, first, size, *to):
    def some(i, _):
        here = pl.ds(pl.multiple_of(i * 16, 16), 16)
        wide = t_ref[here].astype(jnp.float32)
        scale = lax.rsqrt(jnp.mean(wide * wide, -1, keepdims=True) + 1e-6)
        got = (wide * scale * gain).astype(jnp.bfloat16)
        for ref in to:
            ref[here] = got

    lax.fori_loop(first // 16, (first + size) // 16, some, None)


def _gather_matmul(gated, t_ref, gain_ref, *refs):
    (w_refs, refs) = (refs[:2], refs[2:]) if gated else (refs[:3], refs[3:])
    if not gated:
        turn_ref, refs = refs[0], refs[1:]
    (outs, refs) = (refs[:1], refs[1:]) if gated else (refs[:3], refs[3:])
    all_ref, held, raw, mine, lhs, total, stage, w_sem, p_sem, l_sem, o_sem, send, recv, csend, crecv, r_sem = refs
    chip, core, near, sibling = _places()
    tiles = 3
    part = mine.shape[1] // 2

    def hop(i, src, dst, axis):
        return pltpu.make_async_remote_copy(src, dst, send.at[i], recv.at[i], device_id={"tp": near[axis]}, device_id_type=MESH)

    def across(i, src, dst):
        return pltpu.make_async_remote_copy(src, dst, csend.at[i], crecv.at[i], device_id={"tp": sibling}, device_id_type=MESH)

    def rows(unit, whose, at, n):
        return all_ref.at[unit, whose, pl.ds(at, n)]

    hops, cross = {g: [] for g in range(1, 8)}, {g: [] for g in range(1, 8)}
    blocks = [[(0, m, 0, 128) for m in (True, False)]]
    for leg in range(2):
        for p, (at, size, _, _) in enumerate(THIRDS):
            g = 1 + leg * 3 + p
            for n, (one, two, axis) in enumerate(OUT):
                src, unit, way = (rows(one, core, at, size), two, axis) if leg else (mine.at[pl.ds(at, size)], one, one)
                hops[g].append(hop((g - 1) * 3 + n, src, rows(unit, core, at, size), way))
                cross[g].append(across(g * 3 + n, rows(unit, core, at, size), rows(unit, core, at, size)))
            blocks.append([(way[leg], m, at, size) for m in (True, False) for way in OUT])
    for n, (at, size, source, axis) in enumerate(THIRDS):
        hops[7].append(hop(18 + n, rows(source, core, at, size), rows(7, core, at, size), axis))
        cross[7].append(across(21 + n, rows(7, core, at, size), rows(7, core, at, size)))
    blocks += [[(7, m, 0, 128)] for m in (True, False)]
    own = across(0, mine, rows(0, core, 0, 128))
    last = len(blocks) - 1
    early, late = (2, 4) if gated else (5, 5)

    def loads(b, m):
        at, got = 0, []
        for n, (unit, whose, row, size) in enumerate(blocks[b]):
            if whose == m and not (m and unit == 0):
                got.append(pltpu.make_async_copy(rows(unit, core if m else 1 - core, row, size), lhs.at[b % 2, pl.ds(at, size)], l_sem.at[b % 2, n]))
            at += size
        return got

    def arrive(b):
        if b == last:
            return
        for n, c in enumerate(hops[b]):
            c.wait_recv()
            if b < 4:
                hops[b + 3][n].start()
            elif n == b - 4:
                hops[7][n].start()
            cross[b][n].start()
        for c in loads(b, True):
            c.start()

    def settle(b):
        if b == last - 1:
            return
        for c in cross[min(b, 7)]:
            c.wait_recv()
        for c in loads(b, False):
            c.start()

    def staged(t, at, size):
        return stage.at[t, pl.ds(at, size)] if gated else stage.at[t, :, pl.ds(at, size)]

    def stored(b, t):
        at = 0
        for n, (_, _, _, size) in enumerate(blocks[b]):
            pltpu.make_async_copy(staged(t, at, size), staged(t, at, size), o_sem.at[t, n]).wait()
            at += size

    def store(pieces, t, out):
        at = 0
        for n, (unit, whose, row, size) in enumerate(pieces):
            if gated:
                to = out.at[unit, whose, pl.ds(row, size), pl.ds(pl.multiple_of(t * WIDE, WIDE), WIDE)]
            else:
                to = out.at[:, pl.ds(pl.multiple_of((_flips(chip, unit) * 2 + whose) * 128 + row, 16), size)]
            pltpu.make_async_copy(staged(t, at, size), to, o_sem.at[t, n]).start()
            at += size

    def held_load(t):
        return pltpu.make_async_copy(w_refs[0].at[:, pl.ds(t * WIDE, WIDE)] if gated else w_refs[t], held.at[t], w_sem.at[t])

    def part_load(n):
        to = lax.rem(n, 2)
        return pltpu.make_async_copy(w_refs[1].at[:, pl.ds(pl.multiple_of(lax.rem(n, tiles) * WIDE, WIDE), WIDE)], held.at[tiles + to], p_sem.at[to])

    first = pltpu.make_async_copy(t_ref, raw, r_sem)
    first.start()
    partners = (near[X], near[Y], near[Z], sibling)
    barrier = pltpu.get_barrier_semaphore()
    for partner in partners:
        pl.semaphore_signal(barrier, inc=1, device_id={"tp": partner}, device_id_type=MESH)
    first.wait()
    for t in range(tiles):
        held_load(t).start()
        if gated and t < 2:
            part_load(t).start()
    for g, (at, size, _, _) in enumerate(THIRDS, 1):
        _normed(raw, gain_ref[...].astype(jnp.float32)[None], at, size, mine, lhs.at[0])
        if g == 1:
            pl.semaphore_wait(barrier, len(partners))
        for c in hops[g]:
            c.start()
    own.start()
    own.wait_recv()
    for c in loads(0, False):
        c.start()

    for head, many in ((0, 1), (1, 2), (3, 1), (4, 2), (6, 1), (7, 2)):
        tail = head + many - 1
        size = sum(p[3] for p in blocks[head])

        def block(s, _, head=head, many=many, tail=tail, size=size):
            b = head + s
            slot = lax.rem(b, 2)
            pieces, at = [], 0
            for n, ((unit, m, row, z), (_, m1, row1, _)) in enumerate(zip(blocks[head], blocks[tail])):
                if head or not m:
                    got = lhs.at[slot, pl.ds(at, z)]
                    pltpu.make_async_copy(got, got, l_sem.at[slot, n]).wait()
                whose = core if m else 1 - core
                pieces.append((unit, whose if m == m1 else whose + s * (1 - 2 * whose), row if row == row1 else pl.multiple_of(row + s * (row1 - row), 16), z))
                at += z

            def step(j, _):
                t, way = lax.div(j, 2), lax.rem(j, 2)
                n = b * tiles + t
                if head == 0:
                    @pl.when(way == 0)
                    def _():
                        pltpu.make_async_copy(held.at[t], held.at[t], w_sem.at[t]).wait()
                if gated:
                    @pl.when(way == 1)
                    def _():
                        part_load(n).wait()
                    which = (1 - way) * t + way * (tiles + lax.rem(n, 2))
                    total[way, 0:size] = jnp.dot(lhs[slot, 0:size], held[which], preferred_element_type=jnp.float32)

                    @pl.when((way == 1) & (n + 2 < len(blocks) * tiles))
                    def _():
                        part_load(n + 2).start()
                else:
                    @pl.when(way == 0)
                    def _():
                        total[...] = jnp.zeros(total.shape, jnp.float32)
                    here = pl.ds(pl.multiple_of(way * part, part), part)
                    total[0, 0:size] += jnp.dot(lhs[slot, 0:size, here], held[t, here], preferred_element_type=jnp.float32)

                @pl.when(way == 1)
                def _():
                    if head:
                        @pl.when(s == 0)
                        def _():
                            stored(head - 1, t)
                    if many == 2:
                        @pl.when(s == 1)
                        def _():
                            stored(head, t)
                    if gated:
                        stage[t, 0:size] = (jax.nn.silu(total[0, 0:size]) * total[1, 0:size]).astype(jnp.bfloat16)
                        store(pieces, t, outs[0])
                        return

                    @pl.when(t < 2)
                    def _():
                        at = 0
                        for unit, whose, row, z in pieces:
                            shard = _flips(chip, unit) * 2 + whose
                            cos, sin = (turn_ref[i, pl.ds(row, z)] for i in range(2))
                            cos_far, sin_far = (turn_ref[i, pl.ds(128 + shard, 1)] for i in range(2))
                            cos, sin = cos_far * cos - sin_far * sin, sin_far * cos + cos_far * sin
                            for i in range(WIDE // HEAD):
                                flat = total[0, at : at + z, i * HEAD : (i + 1) * HEAD].astype(jnp.bfloat16).astype(jnp.float32)
                                stage[t, i, at : at + z] = (flat * cos + pltpu.roll(flat, HEAD // 2, 1) * sin).astype(jnp.bfloat16)
                            at += z

                    @pl.when(t == 2)
                    def _():
                        for i in range(WIDE // HEAD):
                            stage[t, i, 0:size] = total[0, 0:size, i * HEAD : (i + 1) * HEAD].astype(jnp.bfloat16)

                    for w in range(3):
                        @pl.when(t == w)
                        def _(w=w):
                            store(pieces, t, outs[w])

                for i in range(many):
                    if head + i < last:
                        @pl.when((j == early) & (s == i))
                        def _(i=i):
                            arrive(head + i + 1)

                        @pl.when((j == late) & (s == i))
                        def _(i=i):
                            settle(head + i + 1)

            lax.fori_loop(0, 2 * tiles, step, None)

        lax.fori_loop(0, many, block, None)

    for t in range(tiles):
        stored(last, t)
    own.wait_send()
    for g in hops:
        for c in hops[g] + cross[g]:
            c.wait_send()


def fetched(t, gain, weights, outs, number, turn=None):
    rows, columns = t.shape
    gated = turn is None
    hbm, vmem = pl.BlockSpec(memory_space=pl.ANY), pl.BlockSpec(memory_space=pltpu.VMEM)
    dma, low = pltpu.SemaphoreType.DMA, jnp.bfloat16
    most = 6 * 48
    flops = 32 * rows * columns * sum(w.shape[1] for w in weights)
    return pl.pallas_call(
        functools.partial(_gather_matmul, gated),
        out_shape=[*(jax.ShapeDtypeStruct(shape, low) for shape in outs), jax.ShapeDtypeStruct((8, 2, rows, columns), low)],
        in_specs=[hbm, vmem] + [hbm] * len(weights) + [vmem] * (not gated),
        out_specs=[hbm] * (len(outs) + 1),
        scratch_shapes=[
            pltpu.VMEM((3 + 2 * gated, columns, WIDE), low), pltpu.VMEM((rows, columns), low), pltpu.VMEM((rows, columns), low),
            pltpu.VMEM((2, most, columns), low), pltpu.VMEM((1 + gated, most, WIDE), jnp.float32),
            pltpu.VMEM((3, most, WIDE) if gated else (3, WIDE // HEAD, most, HEAD), low),
            dma((3,)), dma((2,)), dma((2, 6)), dma((3, 6)), dma((21,)), dma((21,)), dma((24,)), dma((24,)), dma(()),
        ],
        compiler_params=pltpu.CompilerParams(collective_id=number, has_side_effects=True, vmem_limit_bytes=KERNEL_VMEM),
        cost_estimate=pl.CostEstimate(flops=flops, transcendentals=0, bytes_accessed=flops // 512),
    )(t, gain, *weights, *(() if gated else (turn,)))[: len(outs)]


IN = {X | Y: Y, Y | Z: Z, Z | X: X, X: X, Y: Y, Z: Z}
TAKES = {X: X | Y, Y: Y | Z, Z: Z | X}
FAR = (7, X | Y, Y | Z, Z | X)
NEAR = (X, Y, Z)
LIVE = 5
STEPS = ((7, 0), (7, 1), *((u, 0) for u in FAR[1:]), *((u, 1) for u in FAR[1:]), *((u, 0) for u in NEAR), *((u, 1) for u in NEAR), (0, 0), (0, 1))


def _attend(q, k, v, first, put, top_s, mix_s, gap_s, scale):
    bk = gap_s.shape[0]
    e = scale * LOG2E
    ones = jnp.ones((8, bk), q.dtype)
    heads = range(q.shape[0])

    top_s[...] = jnp.full(top_s.shape, NEG, jnp.float32)
    mix_s[...] = jnp.zeros(mix_s.shape, jnp.float32)

    def block(j, _):
        here = pl.ds(pl.multiple_of(j * bk, bk), bk)
        seen = gap_s[...] >= j * bk - first
        scores = [_dot(k[i, here], q[i, pl.ds(first, bk)], 1, 1) for i in heads]
        weights, keeps = [], []
        for i, s in zip(heads, scores):
            s = jnp.where(seen, s, HIDDEN)
            old = top_s[i : i + 1]
            top = jnp.maximum(old, s.max(axis=0, keepdims=True))
            top_s[i : i + 1] = top
            weights.append(jnp.exp2((s - top) * e).astype(q.dtype))
            keeps.append(jnp.exp2((old - top) * e))
        for i, p, keep in zip(heads, weights, keeps):
            mix_s[i] = mix_s[i] * keep + _dot(jnp.concatenate([v[i, here].T, ones], axis=0), p, 1, 0)

    lax.fori_loop(0, lax.div(first, bk) + 1, block, None)
    for i in heads:
        put(i, (mix_s[i, :HEAD] * (1 / mix_s[i, HEAD : HEAD + 1])).T.astype(q.dtype))


def _matmul_scatter(heads, *refs):
    a_refs, refs = (refs[:3], refs[3:]) if heads else (refs[:1], refs[1:])
    (w_ref, x_ref, out_ref, last_ref, w, lhs, own, mate, dsend, isend, inc, tin, w_sem, l_sem, t_sem, send, recv, csend, crecv, credit, o_sem) = refs[:21]
    if heads:
        *qkv, top_s, mix_s, gap_s = refs[21:]
    chip, core, near, sibling = _places()
    half = w_ref.shape[1] // 2
    tiles = half // WIDE

    def w_load(t):
        cols = pl.ds(t * WIDE, WIDE) if isinstance(t, int) else pl.ds(pl.multiple_of(t * WIDE, WIDE), WIDE)
        return pltpu.make_async_copy(w_ref.at[:, cols], w.at[:, cols], w_sem.at[t])

    def lhs_loads(n):
        if heads:
            return [pltpu.make_async_copy(a, b, l_sem.at[0, i]) for i, (a, b) in enumerate(zip(a_refs, qkv))] if n == 0 else []
        return [pltpu.make_async_copy(a_refs[0].at[STEPS[n][0], whose], lhs.at[n % 2, pl.ds(i * 128, 128)], l_sem.at[n % 2, i])
                for i, whose in enumerate((core, 1 - core))]

    def attended(unit):
        def put(head, got):
            cols = pl.ds(head * HEAD, HEAD)
            lhs[unit, pl.ds(pl.multiple_of(core * 128, 128), 128), cols] = got[:128]
            lhs[unit, pl.ds(pl.multiple_of(128 - core * 128, 128), 128), cols] = got[128:]

        _attend(*qkv, pl.multiple_of((_flips if isinstance(unit, int) else _flip)(chip, unit) * 256, 256), put, top_s, mix_s, gap_s, HEAD**-0.5)

    def across(n):
        return pltpu.make_async_remote_copy(dsend.at[n % 2], mate.at[n % LIVE], csend.at[n], crecv.at[n], device_id={"tp": sibling}, device_id_type=MESH)

    def place(unit):
        return FAR.index(unit) if unit in FAR else NEAR.index(unit)

    def hop(unit, h, p):
        at, size, _, axis = THIRDS[p]
        axis = axis if unit == 7 else IN[unit]
        to = inc.at[FAR.index(unit)] if unit in FAR else last_ref.at[NEAR.index(unit)]
        return pltpu.make_async_remote_copy(isend.at[place(unit), h, pl.ds(at, size)], to.at[h, pl.ds(at, size)], send.at[unit, h, p],
                                            recv.at[unit, h, p], device_id={"tp": near[axis]}, device_id_type=MESH)

    done, met = {}, set()

    def compute(n):
        unit, h = STEPS[n]
        if n >= LIVE and len(done[n - LIVE]) < 3:
            raise ValueError
        for c in lhs_loads(n):
            c.wait()
        if n + 1 < len(STEPS):
            for c in lhs_loads(n + 1):
                c.start()
        if heads and unit == X and h == 0:
            lax.fori_loop(0, 3, lambda i, _: attended(X - 2 * i + lax.div(i * (i - 1), 2)), None)
        elif heads and unit not in NEAR and unit not in [u for u, _ in STEPS[:n]]:
            attended(unit)
        if n >= 2:
            across(n - 2).wait_send()

        def tile(t, _):
            cols = pl.ds(pl.multiple_of(t * WIDE, WIDE), WIDE)
            from_w = pl.ds(pl.multiple_of(h * half + t * WIDE, WIDE), WIDE)
            if n < 2:
                w_load(h * tiles + t).wait()
            got = jnp.dot(lhs[unit if heads else n % 2], w[:, from_w], preferred_element_type=jnp.float32)
            own[n % LIVE, :, cols] = got[:128]
            dsend[n % 2, :, cols] = got[128:].astype(jnp.bfloat16)

        lax.fori_loop(0, tiles, tile, None)
        if n >= LIVE:
            pl.semaphore_wait(credit.at[n % LIVE], 1)
        across(n).start()

    def finish(n, p):
        unit, h = STEPS[n]
        at, size, third, _ = THIRDS[p]
        if n not in met:
            met.add(n)
            across(n).wait_recv()
        here = pl.ds(at, size)
        source = TAKES.get(unit, 7 if third == unit else None)
        if source is not None:
            hop(source, h, p).wait_recv()
        if unit in NEAR:
            hop(FAR[NEAR.index(unit)], h, p).wait_send()

        def tile(t, _):
            cols = pl.ds(pl.multiple_of(t * WIDE, WIDE), WIDE)
            got = own[n % LIVE, here, cols] + mate[n % LIVE, here, cols].astype(jnp.float32)
            if source is not None:
                got += inc[FAR.index(source), h, here, cols].astype(jnp.float32)
            isend[place(unit), h, here, cols] = got.astype(jnp.bfloat16)

        lax.fori_loop(0, tiles, tile, None)
        hop(unit, h, p).start()
        over(n, p)

    def over(n, p):
        done.setdefault(n, set()).add(p)
        if len(done[n]) == 3 and n + LIVE < len(STEPS):
            pl.semaphore_signal(credit.at[n % LIVE], inc=1, device_id={"tp": sibling}, device_id_type=MESH)

    def last_loads(h, p):
        at, size, _, _ = THIRDS[p]
        to, here = (h * 3 + p) % 2, pl.ds(at, size)
        got = [pltpu.make_async_copy(last_ref.at[i, h, here], tin.at[to, i, 0:size], t_sem.at[to, i]) for i in range(3)]
        return got + [pltpu.make_async_copy(x_ref.at[here, pl.ds(h * half, half)], tin.at[to, 3, 0:size], t_sem.at[to, 3])]

    def fetch_last(h, p):
        for unit in NEAR:
            hop(unit, h, p).wait_recv()
        for c in last_loads(h, p):
            c.start()

    def put(h, p):
        at, size, _, _ = THIRDS[p]
        return pltpu.make_async_copy(isend.at[3, h, pl.ds(at, size)], out_ref.at[pl.ds(at, size), pl.ds(h * half, half)], o_sem.at[h, p])

    def finish_last(h, p):
        at, size, _, _ = THIRDS[p]
        n, here = STEPS.index((0, h)), pl.ds(at, size)
        if n not in met:
            met.add(n)
            across(n).wait_recv()
        hop(FAR[3], h, p).wait_send()
        for c in last_loads(h, p):
            c.wait()

        def tile(t, _):
            cols = pl.ds(pl.multiple_of(t * WIDE, WIDE), WIDE)
            got = own[n % LIVE, here, cols] + mate[n % LIVE, here, cols].astype(jnp.float32)
            for i in range(4):
                got += tin[(h * 3 + p) % 2, i, 0:size, cols].astype(jnp.float32)
            isend[3, h, here, cols] = got.astype(jnp.bfloat16)

        lax.fori_loop(0, tiles, tile, None)
        put(h, p).start()

    for c in lhs_loads(0):
        c.start()
    for t in range(2 * tiles):
        w_load(t).start()
    if heads:
        gap_s[...] = lax.broadcasted_iota(jnp.int32, gap_s.shape, 1) - lax.broadcasted_iota(jnp.int32, gap_s.shape, 0)
    _greet((near[X], near[Y], near[Z], sibling))

    far = ((7, 0), (7, 1), (5, 0), (6, 1), (7, 2))
    for n, sums in (
        (0, ()), (1, ((0, 0), (0, 1), (0, 2))), (2, ((1, 0), (1, 1), (1, 2))), (3, ((2, 1), (2, 2))), (4, ((3, 0), (3, 2))),
        (5, ((4, 0), (4, 1), (2, 0))), (6, ((5, 1), (5, 2), (3, 1))), (7, ((6, 0), (6, 2), (4, 2), *(far if heads else ()))),
        (8, () if heads else far), (9, ()), (10, [(8 + i, p) for p in range(3) for i in range(3)]), (11, ()), (12, ()), (13, ()),
        (14, [(11 + i, p) for p in range(3) for i in range(3)]), (15, ()),
    ):
        compute(n)
        for sum in sums:
            finish(*sum)
    ends = [(h, p) for h in range(2) for p in range(3)]
    fetch_last(*ends[0])
    for i, end in enumerate(ends):
        if i + 1 < len(ends):
            fetch_last(*ends[i + 1])
        finish_last(*end)
    for end in ends:
        put(*end).wait()
        for unit in NEAR:
            hop(unit, *end).wait_send()
    for n in (14, 15):
        across(n).wait_send()


def summed(x, a, w, number):
    rows, columns = x.shape
    depth, half = w.shape[0], columns // 2
    heads = len(a) == 3
    hbm = pl.BlockSpec(memory_space=pl.ANY)
    dma = pltpu.SemaphoreType.DMA
    low, wide = jnp.bfloat16, jnp.float32
    out, _ = pl.pallas_call(
        functools.partial(_matmul_scatter, heads),
        out_shape=[jax.ShapeDtypeStruct((rows, columns), low), jax.ShapeDtypeStruct((3, 2, rows, half), low)],
        in_specs=[hbm] * (len(a) + 2),
        out_specs=[hbm] * 2,
        scratch_shapes=[
            pltpu.VMEM((depth, columns), low), pltpu.VMEM((8 if heads else 2, 2 * rows, depth), low), pltpu.VMEM((LIVE, rows, half), wide),
            pltpu.VMEM((LIVE, rows, half), low), pltpu.VMEM((2, rows, half), low), pltpu.VMEM((4, 2, rows, half), low),
            pltpu.VMEM((4, 2, rows, half), low), pltpu.VMEM((2, 4, 48, half), low),
            dma((columns // WIDE,)), dma((2, 3)), dma((2, 4)), dma((8, 2, 3)), dma((8, 2, 3)), dma((16,)), dma((16,)),
            pltpu.SemaphoreType.REGULAR((LIVE,)), dma((2, 3)),
        ] + ([pltpu.VMEM(t.shape, low) for t in a] + [pltpu.VMEM((4, 256), wide), pltpu.VMEM((4, HEAD + 8, 256), wide), pltpu.VMEM((256, 256), jnp.int32)]
             if heads else []),
        compiler_params=pltpu.CompilerParams(collective_id=number, has_side_effects=True, vmem_limit_bytes=KERNEL_VMEM),
        cost_estimate=pl.CostEstimate(flops=32 * rows * depth * columns, transcendentals=0, bytes_accessed=2 * columns * (depth + 32 * rows)),
    )(*a, w, x)
    return out


def turns():
    place = np.concatenate([np.arange(128), 128 * np.arange(16)])
    angle = place[:, None] * float(THETA) ** (-np.arange(HEAD // 2) / (HEAD // 2))
    cos, sin = np.cos(angle), np.sin(angle)
    return np.stack([np.concatenate([cos, cos], -1), np.concatenate([-sin, sin], -1)]).astype(np.float32)


def solution(mesh):
    def step(x, gain_a, wq, wk, wv, wo, gain_m, w_gate, w_up, w_down):
        rows, wide = x.shape[0], wo.shape[0]
        qkv = fetched(x, gain_a, (wq, wk, wv), [(wide // HEAD, 16 * rows, HEAD)] * 3, 0, turns())
        h = summed(x, qkv, wo, 2)
        (hidden,) = fetched(h, gain_m, (w_gate, w_up), [(8, 2, rows, w_up.shape[1])], 1)
        return summed(h, (hidden,), w_down, 3)

    tokens, columns, rows_of = P(("dp", "tp"), None), P(None, "tp"), P("tp", None)
    return jax.shard_map(
        step,
        mesh=mesh,
        in_specs=(tokens, P(None), columns, columns, columns, rows_of, P(None), columns, columns, rows_of),
        out_specs=tokens,
        check_vma=False,
    )
```

```python
import functools

import jax
import jax.numpy as jnp
import numpy as np
from jax import lax
from jax.experimental import pallas as pl
from jax.experimental.pallas import tpu as pltpu

NEG = -1e30
HIDDEN = 2 * NEG
LOG2E = 1.4426950408889634


def _dot(a, b, ca, cb):
    return lax.dot_general(a, b, (((ca,), (cb,)), ((), ())), preferred_element_type=jnp.float32)


from jax.sharding import PartitionSpec as P

HEAD = 128
THETA = 10000
MESH = pl.DeviceIdType.MESH
KERNEL_VMEM = 66_000_000
X, Y, Z = 4, 2, 1
OUT = ((X, X | Y, Y), (Y, Y | Z, Z), (Z, Z | X, X))
THIRDS = ((0, 48, X | Y, Z), (48, 48, Y | Z, X), (96, 32, Z | X, Y))
WIDE = 512


def _flip(n, bit):
    return n + bit - 2 * bit * lax.rem(lax.div(n, bit), 2)


def _flips(n, bits):
    for bit in (4, 2, 1):
        if bits & bit:
            n = _flip(n, bit)
    return n


def _places():
    me = lax.axis_index("tp")
    chip, core = lax.div(me, 2), lax.rem(me, 2)
    return chip, core, {axis: _flip(me, 2 * axis) for axis in (X, Y, Z)}, _flip(me, 1)


def _greet(partners):
    barrier = pltpu.get_barrier_semaphore()
    for partner in partners:
        pl.semaphore_signal(barrier, inc=1, device_id={"tp": partner}, device_id_type=MESH)
    pl.semaphore_wait(barrier, len(partners))


def _normed(t_ref, gain, first, size, *to):
    def some(i, _):
        here = pl.ds(pl.multiple_of(i * 16, 16), 16)
        wide = t_ref[here].astype(jnp.float32)
        scale = lax.rsqrt(jnp.mean(wide * wide, -1, keepdims=True) + 1e-6)
        got = (wide * scale * gain).astype(jnp.bfloat16)
        for ref in to:
            ref[here] = got

    lax.fori_loop(first // 16, (first + size) // 16, some, None)


def _gather_matmul(gated, t_ref, gain_ref, *refs):
    (w_refs, refs) = (refs[:2], refs[2:]) if gated else (refs[:3], refs[3:])
    if not gated:
        turn_ref, refs = refs[0], refs[1:]
    (outs, refs) = (refs[:1], refs[1:]) if gated else (refs[:3], refs[3:])
    all_ref, held, raw, mine, lhs, total, stage, w_sem, p_sem, l_sem, o_sem, send, recv, csend, crecv, r_sem = refs
    chip, core, near, sibling = _places()
    tiles = 3
    part = mine.shape[1] // 2

    def hop(i, src, dst, axis):
        return pltpu.make_async_remote_copy(src, dst, send.at[i], recv.at[i], device_id={"tp": near[axis]}, device_id_type=MESH)

    def across(i, src, dst):
        return pltpu.make_async_remote_copy(src, dst, csend.at[i], crecv.at[i], device_id={"tp": sibling}, device_id_type=MESH)

    def rows(unit, whose, at, n):
        return all_ref.at[unit, whose, pl.ds(at, n)]

    hops, cross = {g: [] for g in range(1, 8)}, {g: [] for g in range(1, 8)}
    blocks = [[(0, m, 0, 128) for m in (True, False)]]
    for leg in range(2):
        for p, (at, size, _, _) in enumerate(THIRDS):
            g = 1 + leg * 3 + p
            for n, (one, two, axis) in enumerate(OUT):
                src, unit, way = (rows(one, core, at, size), two, axis) if leg else (mine.at[pl.ds(at, size)], one, one)
                hops[g].append(hop((g - 1) * 3 + n, src, rows(unit, core, at, size), way))
                cross[g].append(across(g * 3 + n, rows(unit, core, at, size), rows(unit, core, at, size)))
            blocks.append([(way[leg], m, at, size) for m in (True, False) for way in OUT])
    for n, (at, size, source, axis) in enumerate(THIRDS):
        hops[7].append(hop(18 + n, rows(source, core, at, size), rows(7, core, at, size), axis))
        cross[7].append(across(21 + n, rows(7, core, at, size), rows(7, core, at, size)))
    blocks += [[(7, m, 0, 128)] for m in (True, False)]
    own = across(0, mine, rows(0, core, 0, 128))
    last = len(blocks) - 1
    early, late = (2, 4) if gated else (5, 5)

    def loads(b, m):
        at, got = 0, []
        for n, (unit, whose, row, size) in enumerate(blocks[b]):
            if whose == m and not (m and unit == 0):
                got.append(pltpu.make_async_copy(rows(unit, core if m else 1 - core, row, size), lhs.at[b % 2, pl.ds(at, size)], l_sem.at[b % 2, n]))
            at += size
        return got

    def arrive(b):
        if b == last:
            return
        for n, c in enumerate(hops[b]):
            c.wait_recv()
            if b < 4:
                hops[b + 3][n].start()
            elif n == b - 4:
                hops[7][n].start()
            cross[b][n].start()
        for c in loads(b, True):
            c.start()

    def settle(b):
        if b == last - 1:
            return
        for c in cross[min(b, 7)]:
            c.wait_recv()
        for c in loads(b, False):
            c.start()

    def staged(t, at, size):
        return stage.at[t, pl.ds(at, size)] if gated else stage.at[t, :, pl.ds(at, size)]

    def stored(b, t):
        at = 0
        for n, (_, _, _, size) in enumerate(blocks[b]):
            pltpu.make_async_copy(staged(t, at, size), staged(t, at, size), o_sem.at[t, n]).wait()
            at += size

    def store(pieces, t, out):
        at = 0
        for n, (unit, whose, row, size) in enumerate(pieces):
            if gated:
                to = out.at[unit, whose, pl.ds(row, size), pl.ds(pl.multiple_of(t * WIDE, WIDE), WIDE)]
            else:
                to = out.at[:, pl.ds(pl.multiple_of((_flips(chip, unit) * 2 + whose) * 128 + row, 16), size)]
            pltpu.make_async_copy(staged(t, at, size), to, o_sem.at[t, n]).start()
            at += size

    def held_load(t):
        return pltpu.make_async_copy(w_refs[0].at[:, pl.ds(t * WIDE, WIDE)] if gated else w_refs[t], held.at[t], w_sem.at[t])

    def part_load(n):
        to = lax.rem(n, 2)
        return pltpu.make_async_copy(w_refs[1].at[:, pl.ds(pl.multiple_of(lax.rem(n, tiles) * WIDE, WIDE), WIDE)], held.at[tiles + to], p_sem.at[to])

    first = pltpu.make_async_copy(t_ref, raw, r_sem)
    first.start()
    partners = (near[X], near[Y], near[Z], sibling)
    barrier = pltpu.get_barrier_semaphore()
    for partner in partners:
        pl.semaphore_signal(barrier, inc=1, device_id={"tp": partner}, device_id_type=MESH)
    first.wait()
    for t in range(tiles):
        held_load(t).start()
        if gated and t < 2:
            part_load(t).start()
    for g, (at, size, _, _) in enumerate(THIRDS, 1):
        _normed(raw, gain_ref[...].astype(jnp.float32)[None], at, size, mine, lhs.at[0])
        if g == 1:
            pl.semaphore_wait(barrier, len(partners))
        for c in hops[g]:
            c.start()
    own.start()
    own.wait_recv()
    for c in loads(0, False):
        c.start()

    for head, many in ((0, 1), (1, 2), (3, 1), (4, 2), (6, 1), (7, 2)):
        tail = head + many - 1
        size = sum(p[3] for p in blocks[head])

        def block(s, _, head=head, many=many, tail=tail, size=size):
            b = head + s
            slot = lax.rem(b, 2)
            pieces, at = [], 0
            for n, ((unit, m, row, z), (_, m1, row1, _)) in enumerate(zip(blocks[head], blocks[tail])):
                if head or not m:
                    got = lhs.at[slot, pl.ds(at, z)]
                    pltpu.make_async_copy(got, got, l_sem.at[slot, n]).wait()
                whose = core if m else 1 - core
                pieces.append((unit, whose if m == m1 else whose + s * (1 - 2 * whose), row if row == row1 else pl.multiple_of(row + s * (row1 - row), 16), z))
                at += z

            def step(j, _):
                t, way = lax.div(j, 2), lax.rem(j, 2)
                n = b * tiles + t
                if head == 0:
                    @pl.when(way == 0)
                    def _():
                        pltpu.make_async_copy(held.at[t], held.at[t], w_sem.at[t]).wait()
                if gated:
                    @pl.when(way == 1)
                    def _():
                        part_load(n).wait()
                    which = (1 - way) * t + way * (tiles + lax.rem(n, 2))
                    total[way, 0:size] = jnp.dot(lhs[slot, 0:size], held[which], preferred_element_type=jnp.float32)

                    @pl.when((way == 1) & (n + 2 < len(blocks) * tiles))
                    def _():
                        part_load(n + 2).start()
                else:
                    @pl.when(way == 0)
                    def _():
                        total[...] = jnp.zeros(total.shape, jnp.float32)
                    here = pl.ds(pl.multiple_of(way * part, part), part)
                    total[0, 0:size] += jnp.dot(lhs[slot, 0:size, here], held[t, here], preferred_element_type=jnp.float32)

                @pl.when(way == 1)
                def _():
                    if head:
                        @pl.when(s == 0)
                        def _():
                            stored(head - 1, t)
                    if many == 2:
                        @pl.when(s == 1)
                        def _():
                            stored(head, t)
                    if gated:
                        stage[t, 0:size] = (jax.nn.silu(total[0, 0:size]) * total[1, 0:size]).astype(jnp.bfloat16)
                        store(pieces, t, outs[0])
                        return

                    @pl.when(t < 2)
                    def _():
                        at = 0
                        for unit, whose, row, z in pieces:
                            shard = _flips(chip, unit) * 2 + whose
                            cos, sin = (turn_ref[i, pl.ds(row, z)] for i in range(2))
                            cos_far, sin_far = (turn_ref[i, pl.ds(128 + shard, 1)] for i in range(2))
                            cos, sin = cos_far * cos - sin_far * sin, sin_far * cos + cos_far * sin
                            for i in range(WIDE // HEAD):
                                flat = total[0, at : at + z, i * HEAD : (i + 1) * HEAD].astype(jnp.bfloat16).astype(jnp.float32)
                                stage[t, i, at : at + z] = (flat * cos + pltpu.roll(flat, HEAD // 2, 1) * sin).astype(jnp.bfloat16)
                            at += z

                    @pl.when(t == 2)
                    def _():
                        for i in range(WIDE // HEAD):
                            stage[t, i, 0:size] = total[0, 0:size, i * HEAD : (i + 1) * HEAD].astype(jnp.bfloat16)

                    for w in range(3):
                        @pl.when(t == w)
                        def _(w=w):
                            store(pieces, t, outs[w])

                for i in range(many):
                    if head + i < last:
                        @pl.when((j == early) & (s == i))
                        def _(i=i):
                            arrive(head + i + 1)

                        @pl.when((j == (late if head < 7 else 4)) & (s == i))
                        def _(i=i):
                            settle(head + i + 1)

            lax.fori_loop(0, 2 * tiles, step, None)

        lax.fori_loop(0, many, block, None)

    for t in range(tiles):
        stored(last, t)
    own.wait_send()
    for g in hops:
        for c in hops[g] + cross[g]:
            c.wait_send()


def fetched(t, gain, weights, outs, number, turn=None):
    rows, columns = t.shape
    gated = turn is None
    hbm, vmem = pl.BlockSpec(memory_space=pl.ANY), pl.BlockSpec(memory_space=pltpu.VMEM)
    dma, low = pltpu.SemaphoreType.DMA, jnp.bfloat16
    most = 6 * 48
    flops = 32 * rows * columns * sum(w.shape[1] for w in weights)
    return pl.pallas_call(
        functools.partial(_gather_matmul, gated),
        out_shape=[*(jax.ShapeDtypeStruct(shape, low) for shape in outs), jax.ShapeDtypeStruct((8, 2, rows, columns), low)],
        in_specs=[hbm, vmem] + [hbm] * len(weights) + [vmem] * (not gated),
        out_specs=[hbm] * (len(outs) + 1),
        scratch_shapes=[
            pltpu.VMEM((3 + 2 * gated, columns, WIDE), low), pltpu.VMEM((rows, columns), low), pltpu.VMEM((rows, columns), low),
            pltpu.VMEM((2, most, columns), low), pltpu.VMEM((1 + gated, most, WIDE), jnp.float32),
            pltpu.VMEM((3, most, WIDE) if gated else (3, WIDE // HEAD, most, HEAD), low),
            dma((3,)), dma((2,)), dma((2, 6)), dma((3, 6)), dma((21,)), dma((21,)), dma((24,)), dma((24,)), dma(()),
        ],
        compiler_params=pltpu.CompilerParams(collective_id=number, has_side_effects=True, vmem_limit_bytes=KERNEL_VMEM),
        cost_estimate=pl.CostEstimate(flops=flops, transcendentals=0, bytes_accessed=flops // 512),
    )(t, gain, *weights, *(() if gated else (turn,)))[: len(outs)]


IN = {X | Y: Y, Y | Z: Z, Z | X: X, X: X, Y: Y, Z: Z}
TAKES = {X: X | Y, Y: Y | Z, Z: Z | X}
FAR = (7, X | Y, Y | Z, Z | X)
NEAR = (X, Y, Z)
LIVE = 5
STEPS = ((7, 0), (7, 1), *((u, 0) for u in FAR[1:]), *((u, 1) for u in FAR[1:]), *((u, 0) for u in NEAR), *((u, 1) for u in NEAR), (0, 0), (0, 1))


def _attend(q, k, v, first, put, top_s, mix_s, gap_s, scale):
    bk = gap_s.shape[0]
    e = scale * LOG2E
    ones = jnp.ones((8, bk), q.dtype)
    heads = range(q.shape[0])

    top_s[...] = jnp.full(top_s.shape, NEG, jnp.float32)
    mix_s[...] = jnp.zeros(mix_s.shape, jnp.float32)

    def block(j, _):
        here = pl.ds(pl.multiple_of(j * bk, bk), bk)
        seen = gap_s[...] >= j * bk - first
        scores = [_dot(k[i, here], q[i, pl.ds(first, bk)], 1, 1) for i in heads]
        weights, keeps = [], []
        for i, s in zip(heads, scores):
            s = jnp.where(seen, s, HIDDEN)
            old = top_s[i : i + 1]
            top = jnp.maximum(old, s.max(axis=0, keepdims=True))
            top_s[i : i + 1] = top
            weights.append(jnp.exp2((s - top) * e).astype(q.dtype))
            keeps.append(jnp.exp2((old - top) * e))
        for i, p, keep in zip(heads, weights, keeps):
            mix_s[i] = mix_s[i] * keep + _dot(jnp.concatenate([v[i, here].T, ones], axis=0), p, 1, 0)

    lax.fori_loop(0, lax.div(first, bk) + 1, block, None)
    for i in heads:
        put(i, (mix_s[i, :HEAD] * (1 / mix_s[i, HEAD : HEAD + 1])).T.astype(q.dtype))


def _matmul_scatter(heads, *refs):
    a_refs, refs = (refs[:3], refs[3:]) if heads else (refs[:1], refs[1:])
    (w_ref, x_ref, out_ref, last_ref, w, lhs, own, mate, dsend, isend, inc, tin, w_sem, l_sem, t_sem, send, recv, csend, crecv, credit, o_sem) = refs[:21]
    if heads:
        *qkv, top_s, mix_s, gap_s = refs[21:]
    chip, core, near, sibling = _places()
    half = w_ref.shape[1] // 2
    tiles = half // WIDE

    def w_load(t):
        cols = pl.ds(t * WIDE, WIDE) if isinstance(t, int) else pl.ds(pl.multiple_of(t * WIDE, WIDE), WIDE)
        return pltpu.make_async_copy(w_ref.at[:, cols], w.at[:, cols], w_sem.at[t])

    def lhs_loads(n):
        if heads:
            return [pltpu.make_async_copy(a, b, l_sem.at[0, i]) for i, (a, b) in enumerate(zip(a_refs, qkv))] if n == 0 else []
        return [pltpu.make_async_copy(a_refs[0].at[STEPS[n][0], whose], lhs.at[n % 2, pl.ds(i * 128, 128)], l_sem.at[n % 2, i])
                for i, whose in enumerate((core, 1 - core))]

    def attended(unit):
        def put(head, got):
            cols = pl.ds(head * HEAD, HEAD)
            lhs[unit, pl.ds(pl.multiple_of(core * 128, 128), 128), cols] = got[:128]
            lhs[unit, pl.ds(pl.multiple_of(128 - core * 128, 128), 128), cols] = got[128:]

        _attend(*qkv, pl.multiple_of((_flips if isinstance(unit, int) else _flip)(chip, unit) * 256, 256), put, top_s, mix_s, gap_s, HEAD**-0.5)

    def across(n):
        return pltpu.make_async_remote_copy(dsend.at[n % 2], mate.at[n % LIVE], csend.at[n], crecv.at[n], device_id={"tp": sibling}, device_id_type=MESH)

    def place(unit):
        return FAR.index(unit) if unit in FAR else NEAR.index(unit)

    def hop(unit, h, p):
        at, size, _, axis = THIRDS[p]
        axis = axis if unit == 7 else IN[unit]
        to = inc.at[FAR.index(unit)] if unit in FAR else last_ref.at[NEAR.index(unit)]
        return pltpu.make_async_remote_copy(isend.at[place(unit), h, pl.ds(at, size)], to.at[h, pl.ds(at, size)], send.at[unit, h, p],
                                            recv.at[unit, h, p], device_id={"tp": near[axis]}, device_id_type=MESH)

    done, met = {}, set()

    def compute(n):
        unit, h = STEPS[n]
        if n >= LIVE and len(done[n - LIVE]) < 3:
            raise ValueError
        for c in lhs_loads(n):
            c.wait()
        if n + 1 < len(STEPS):
            for c in lhs_loads(n + 1):
                c.start()
        if heads and unit == X and h == 0:
            lax.fori_loop(0, 3, lambda i, _: attended(X - 2 * i + lax.div(i * (i - 1), 2)), None)
        elif heads and unit not in NEAR and unit not in [u for u, _ in STEPS[:n]]:
            attended(unit)
        if n >= 2:
            across(n - 2).wait_send()

        def tile(t, _):
            cols = pl.ds(pl.multiple_of(t * WIDE, WIDE), WIDE)
            from_w = pl.ds(pl.multiple_of(h * half + t * WIDE, WIDE), WIDE)
            if n < 2:
                w_load(h * tiles + t).wait()
            got = jnp.dot(lhs[unit if heads else n % 2], w[:, from_w], preferred_element_type=jnp.float32)
            own[n % LIVE, :, cols] = got[:128]
            dsend[n % 2, :, cols] = got[128:].astype(jnp.bfloat16)

        lax.fori_loop(0, tiles, tile, None)
        if n >= LIVE:
            pl.semaphore_wait(credit.at[n % LIVE], 1)
        across(n).start()

    def finish(n, p):
        unit, h = STEPS[n]
        at, size, third, _ = THIRDS[p]
        if n not in met:
            met.add(n)
            across(n).wait_recv()
        here = pl.ds(at, size)
        source = TAKES.get(unit, 7 if third == unit else None)
        if source is not None:
            hop(source, h, p).wait_recv()
        if unit in NEAR:
            hop(FAR[NEAR.index(unit)], h, p).wait_send()

        def tile(t, _):
            cols = pl.ds(pl.multiple_of(t * WIDE, WIDE), WIDE)
            got = own[n % LIVE, here, cols] + mate[n % LIVE, here, cols].astype(jnp.float32)
            if source is not None:
                got += inc[FAR.index(source), h, here, cols].astype(jnp.float32)
            isend[place(unit), h, here, cols] = got.astype(jnp.bfloat16)

        lax.fori_loop(0, tiles, tile, None)
        hop(unit, h, p).start()
        over(n, p)

    def over(n, p):
        done.setdefault(n, set()).add(p)
        if len(done[n]) == 3 and n + LIVE < len(STEPS):
            pl.semaphore_signal(credit.at[n % LIVE], inc=1, device_id={"tp": sibling}, device_id_type=MESH)

    def last_loads(h, p):
        at, size, _, _ = THIRDS[p]
        to, here = (h * 3 + p) % 2, pl.ds(at, size)
        got = [pltpu.make_async_copy(last_ref.at[i, h, here], tin.at[to, i, 0:size], t_sem.at[to, i]) for i in range(3)]
        return got + [pltpu.make_async_copy(x_ref.at[here, pl.ds(h * half, half)], tin.at[to, 3, 0:size], t_sem.at[to, 3])]

    def fetch_last(h, p):
        for unit in NEAR:
            hop(unit, h, p).wait_recv()
        for c in last_loads(h, p):
            c.start()

    def put(h, p):
        at, size, _, _ = THIRDS[p]
        return pltpu.make_async_copy(isend.at[3, h, pl.ds(at, size)], out_ref.at[pl.ds(at, size), pl.ds(h * half, half)], o_sem.at[h, p])

    def finish_last(h, p):
        at, size, _, _ = THIRDS[p]
        n, here = STEPS.index((0, h)), pl.ds(at, size)
        if n not in met:
            met.add(n)
            across(n).wait_recv()
        hop(FAR[3], h, p).wait_send()
        for c in last_loads(h, p):
            c.wait()

        def tile(t, _):
            cols = pl.ds(pl.multiple_of(t * WIDE, WIDE), WIDE)
            got = own[n % LIVE, here, cols] + mate[n % LIVE, here, cols].astype(jnp.float32)
            for i in range(4):
                got += tin[(h * 3 + p) % 2, i, 0:size, cols].astype(jnp.float32)
            isend[3, h, here, cols] = got.astype(jnp.bfloat16)

        lax.fori_loop(0, tiles, tile, None)
        put(h, p).start()

    for c in lhs_loads(0):
        c.start()
    for t in range(2 * tiles):
        w_load(t).start()
    if heads:
        gap_s[...] = lax.broadcasted_iota(jnp.int32, gap_s.shape, 1) - lax.broadcasted_iota(jnp.int32, gap_s.shape, 0)
    _greet((near[X], near[Y], near[Z], sibling))

    far = ((7, 0), (7, 1), (5, 0), (6, 1), (7, 2))
    for n, sums in (
        (0, ()), (1, ((0, 0), (0, 1), (0, 2))), (2, ((1, 0), (1, 1), (1, 2))), (3, ((2, 1), (2, 2))), (4, ((3, 0), (3, 2), (4, 0), (4, 1))),
        (5, ((2, 0),)), (6, ((5, 1), (5, 2), (3, 1))), (7, ((6, 0), (6, 2), (4, 2), *(far if heads else ()))),
        (8, () if heads else far), (9, ()), (10, [(8 + i, p) for p in range(3) for i in range(3)]), (11, ()), (12, ()), (13, ()),
        (14, [(11 + i, p) for p in range(3) for i in range(3)]), (15, ()),
    ):
        compute(n)
        for sum in sums:
            finish(*sum)
    ends = [(h, p) for h in range(2) for p in range(3)]
    fetch_last(*ends[0])
    for i, end in enumerate(ends):
        if i + 1 < len(ends):
            fetch_last(*ends[i + 1])
        finish_last(*end)
    for end in ends:
        put(*end).wait()
        for unit in NEAR:
            hop(unit, *end).wait_send()
    for n in (14, 15):
        across(n).wait_send()


def summed(x, a, w, number):
    rows, columns = x.shape
    depth, half = w.shape[0], columns // 2
    heads = len(a) == 3
    hbm = pl.BlockSpec(memory_space=pl.ANY)
    dma = pltpu.SemaphoreType.DMA
    low, wide = jnp.bfloat16, jnp.float32
    out, _ = pl.pallas_call(
        functools.partial(_matmul_scatter, heads),
        out_shape=[jax.ShapeDtypeStruct((rows, columns), low), jax.ShapeDtypeStruct((3, 2, rows, half), low)],
        in_specs=[hbm] * (len(a) + 2),
        out_specs=[hbm] * 2,
        scratch_shapes=[
            pltpu.VMEM((depth, columns), low), pltpu.VMEM((8 if heads else 2, 2 * rows, depth), low), pltpu.VMEM((LIVE, rows, half), wide),
            pltpu.VMEM((LIVE, rows, half), low), pltpu.VMEM((2, rows, half), low), pltpu.VMEM((4, 2, rows, half), low),
            pltpu.VMEM((4, 2, rows, half), low), pltpu.VMEM((2, 4, 48, half), low),
            dma((columns // WIDE,)), dma((2, 3)), dma((2, 4)), dma((8, 2, 3)), dma((8, 2, 3)), dma((16,)), dma((16,)),
            pltpu.SemaphoreType.REGULAR((LIVE,)), dma((2, 3)),
        ] + ([pltpu.VMEM(t.shape, low) for t in a] + [pltpu.VMEM((4, 256), wide), pltpu.VMEM((4, HEAD + 8, 256), wide), pltpu.VMEM((256, 256), jnp.int32)]
             if heads else []),
        compiler_params=pltpu.CompilerParams(collective_id=number, has_side_effects=True, vmem_limit_bytes=KERNEL_VMEM),
        cost_estimate=pl.CostEstimate(flops=32 * rows * depth * columns, transcendentals=0, bytes_accessed=2 * columns * (depth + 32 * rows)),
    )(*a, w, x)
    return out


def turns():
    place = np.concatenate([np.arange(128), 128 * np.arange(16)])
    angle = place[:, None] * float(THETA) ** (-np.arange(HEAD // 2) / (HEAD // 2))
    cos, sin = np.cos(angle), np.sin(angle)
    return np.stack([np.concatenate([cos, cos], -1), np.concatenate([-sin, sin], -1)]).astype(np.float32)


def solution(mesh):
    def step(x, gain_a, wq, wk, wv, wo, gain_m, w_gate, w_up, w_down):
        rows, wide = x.shape[0], wo.shape[0]
        qkv = fetched(x, gain_a, (wq, wk, wv), [(wide // HEAD, 16 * rows, HEAD)] * 3, 0, turns())
        h = summed(x, qkv, wo, 2)
        (hidden,) = fetched(h, gain_m, (w_gate, w_up), [(8, 2, rows, w_up.shape[1])], 1)
        return summed(h, (hidden,), w_down, 3)

    tokens, columns, rows_of = P(("dp", "tp"), None), P(None, "tp"), P("tp", None)
    return jax.shard_map(
        step,
        mesh=mesh,
        in_specs=(tokens, P(None), columns, columns, columns, rows_of, P(None), columns, columns, rows_of),
        out_specs=tokens,
        check_vma=False,
    )
```
